512 devices in a mesh: groups: 2 (over y), vel: 32 (over z), space: 4 (over x), spec: 2 (over core).
Axes of the slice: x: 4, y: 2, z: 32, core: 2. Of those that a mesh axis runs over, the one named last changes fastest.
The devices are a block of a 4x16x32 slice.
Arguments:
- distribution: float32 [2, 64, 64, 32768], P('spec', ('groups', 'space'), None, 'vel'), parts along dimension 1, may hold values from 0.25 to 4
- vel_order: int32 [32768], P('vel'), may hold values from 0 to 32767, each once
- species_mass: int32 [2], P('spec'), may hold values from 1 to 8
- wall_mask: int32 [64, 2], P(('groups', 'space')), parts along dimension 0, may hold values 0 or 1
- inflow_mask: int32 [64, 2], P(('groups', 'space')), parts along dimension 0, may hold values 0 or 1
Outputs:
- updated: float32 [2, 64, 64, 32768], P('spec', ('groups', 'space'), None, 'vel'), parts along dimension 1
The draws below stay inside these ranges and needn't reach their ends.
There are 2 independent parts, one for each index of `groups`. The reference program is written for one: setup_inputs(seed, part) draws one part's arguments, and reference() takes and returns one part's arrays. A program takes and returns all parts, laid end to end along the dimension named above; an argument that names none is the same for every part. Nothing has to cross between parts.
Inputs may be any that keep to these rules, and one draw needn't show every extreme that they name: `vel_order`: each number from 0 to 32767 appears once.
All inputs are finite; a program needn't handle non-finite values. No bound on the sum of `wall_mask` or of `inflow_mask` on one device may be relied on, other than what follows from the above.
Results may differ from the reference program's by a relative error of at most 0.0001.
Values sent between devices are 32-bit elements; how exact they have to be, the bound alone decides.
A program may use at most 64 MiB of HBM per device.

```python
import math
import jax
import jax.numpy as jnp
from jax import lax

NV = 32
NY = 64
NVEL = 32768
NX = 32


def set_ends(array, rng, smallest, high):
    index_at = [jax.random.randint(jax.random.fold_in(rng, axis), (), 0, length) for axis, length in enumerate(array.shape)]
    main_axis = array.shape.index(max(array.shape))
    beside = index_at[:main_axis] + [(index_at[main_axis] + 1) % array.shape[main_axis]] + index_at[main_axis + 1:]
    return array.at[tuple(index_at)].set(smallest).at[tuple(beside)].set(high)


def levels(key, extent, split, low, top_value):
    level = 1.0
    for position, parts in split:
        heights = jax.random.uniform(jax.random.fold_in(jax.random.fold_in(key, 6), position), (parts,), jnp.float32, low / len(split), top_value / len(split))
        level = level * jnp.repeat(jnp.exp(heights), extent[position] // parts).reshape((-1,) + (1,) * (len(extent) - 1 - position))
    return level


def setup_inputs(seed: int = 0, part: int = 0) -> dict:
    keys = jax.random.split(jax.random.key(seed), 6)
    part_splits = jax.random.split(jax.random.fold_in(keys[5], part), 6)
    distribution = jnp.clip(jnp.exp(math.log(4.0) - 2.7725887 * jax.random.uniform(part_splits[0], (2, NX, NY, NVEL), jnp.float32) ** levels(part_splits[0], (2, NX, NY, NVEL), ((0, 2), (1, 4), (3, 32)), -0.2, 0.2)), 0.25, 4.0)
    vel_order = jax.random.permutation(keys[1], NVEL).astype(jnp.int32)
    species_mass = jax.random.randint(keys[2], (2,), 1, 9).astype(jnp.int32)
    wall_mask = set_ends((jax.random.randint(part_splits[3], (NX, 2), 0, 2) < 1).astype(jnp.int32), jax.random.fold_in(part_splits[3], 1), 0, 1)
    inflow_mask = set_ends((jax.random.randint(part_splits[4], (NX, 2), 0, 2) < 1).astype(jnp.int32), jax.random.fold_in(part_splits[4], 1), 0, 1)
    return {"distribution": distribution, "vel_order": vel_order, "species_mass": species_mass, "wall_mask": wall_mask, "inflow_mask": inflow_mask}


TIME_STEP = 0.1
RAREFACTION = 0.5
PORT_DENSITY = 1.0
HALF_RANGE = 4.5
PRECISE = lax.Precision.HIGHEST

def lattice(lattice_ids, molecule_weight):
    spacing = 2.0 * HALF_RANGE / (NV - 1) / jnp.sqrt(molecule_weight)
    centre = (NV - 1) / 2.0
    index_a = (lattice_ids // (NV * NV)).astype(jnp.float32)
    index_b = (lattice_ids // NV % NV).astype(jnp.float32)
    index_e = (lattice_ids % NV).astype(jnp.float32)
    return ((index_a - centre) * spacing, (index_b - centre) * spacing, (index_e - centre) * spacing, spacing)

def features(speed_x, speed_y, speed_z, molecule_weight):
    square = speed_x * speed_x + speed_y * speed_y + speed_z * speed_z
    unity = jnp.ones_like(speed_x)
    moment_rows = jnp.stack([unity, molecule_weight * unity, molecule_weight * speed_x, molecule_weight * speed_y, molecule_weight * speed_z, 0.5 * molecule_weight * square])
    shape_rows = jnp.stack([unity, speed_x, speed_y, speed_z, square])
    return (moment_rows, shape_rows, square)

def wall_law(square, spacing, molecule_weight):
    return jnp.exp(jnp.log(NVEL * spacing ** 3) + 1.5 * jnp.log(molecule_weight / (2.0 * jnp.pi)) - 0.5 * molecule_weight * square)

def wall_scale(molecule_weight):
    all_points = jnp.arange(NVEL, dtype=jnp.int32)
    speed_x, speed_y, speed_z, spacing = lattice(all_points, molecule_weight)
    square = speed_x * speed_x + speed_y * speed_y + speed_z * speed_z
    return jnp.sum(jnp.maximum(speed_y, 0.0) * wall_law(square, spacing, molecule_weight)) / NVEL

def mixture(first_moments, second_moments):
    blended_gas_sums_all = first_moments + second_moments
    count_per_volume = blended_gas_sums_all[0]
    component_weight_per_volume = blended_gas_sums_all[1]
    mean_drift_first = blended_gas_sums_all[2] / component_weight_per_volume
    mean_drift_second = blended_gas_sums_all[3] / component_weight_per_volume
    mean_drift_third = blended_gas_sums_all[4] / component_weight_per_volume
    motion_work_content = mean_drift_first * mean_drift_first + mean_drift_second * mean_drift_second + mean_drift_third * mean_drift_third
    cellwise_thermal_level = 2.0 / 3.0 * (blended_gas_sums_all[5] - 0.5 * component_weight_per_volume * motion_work_content) / count_per_volume
    return (mean_drift_first, mean_drift_second, mean_drift_third, cellwise_thermal_level, count_per_volume / RAREFACTION)

def coefficients(own_moments, blended_gas_mean, molecule_weight, spacing):
    mean_drift_first, mean_drift_second, mean_drift_third, cellwise_thermal_level, collision_pace = blended_gas_mean
    reciprocal_crowding = molecule_weight / cellwise_thermal_level
    motion_work_content = mean_drift_first * mean_drift_first + mean_drift_second * mean_drift_second + mean_drift_third * mean_drift_third
    leading = jnp.log(own_moments[0]) + jnp.log(NVEL * spacing ** 3) + 1.5 * jnp.log(reciprocal_crowding / (2.0 * jnp.pi)) - 0.5 * reciprocal_crowding * motion_work_content
    return jnp.stack([leading, reciprocal_crowding * mean_drift_first, reciprocal_crowding * mean_drift_second, reciprocal_crowding * mean_drift_third, -0.5 * reciprocal_crowding])

def collide(dist_rows, coeffs, collision_pace, shape_rows):
    exponent = lax.dot_general(coeffs, shape_rows, (((0,), (0,)), ((), ())), precision=PRECISE, preferred_element_type=jnp.float32)
    return dist_rows + TIME_STEP * collision_pace[:, None] * (jnp.exp(exponent) - dist_rows)

def stream(collided, left_cells, right_cells, ghost_low, ghost_high, speed_x, speed_y):
    below_cells = jnp.concatenate([ghost_low[:, None, :], collided[:, :-1, :]], axis=1)
    above_cells = jnp.concatenate([collided[:, 1:, :], ghost_high[:, None, :]], axis=1)
    plus_x = jnp.maximum(speed_x, 0.0)
    minus_x = jnp.minimum(speed_x, 0.0)
    plus_y = jnp.maximum(speed_y, 0.0)
    minus_y = jnp.minimum(speed_y, 0.0)
    change = plus_x * (collided - left_cells) + minus_x * (right_cells - collided) + plus_y * (collided - below_cells) + minus_y * (above_cells - collided)
    return collided - TIME_STEP * change

def reference(distribution, vel_order, species_mass, wall_mask, inflow_mask):
    masses = species_mass.astype(jnp.float32)
    cell_count = NX * NY
    moments = []
    incident = []
    for species in range(2):
        speed_x, speed_y, speed_z, spacing = lattice(vel_order, masses[species])
        moment_rows, shape_rows, square = features(speed_x, speed_y, speed_z, masses[species])
        flat_dist = distribution[species].reshape(cell_count, NVEL)
        moments.append(lax.dot_general(moment_rows, flat_dist, (((1,), (1,)), ((), ())), precision=PRECISE, preferred_element_type=jnp.float32) / NVEL)
        low_flux = jnp.dot(distribution[species][:, 0, :], jnp.maximum(-speed_y, 0.0), precision=PRECISE) / NVEL
        high_flux = jnp.dot(distribution[species][:, NY - 1, :], jnp.maximum(speed_y, 0.0), precision=PRECISE) / NVEL
        incident.append(jnp.stack([low_flux, high_flux], axis=1))
    blended_gas_mean = mixture(moments[0], moments[1])
    wall_weight = wall_mask.astype(jnp.float32)
    inflow_weight = inflow_mask.astype(jnp.float32)
    results = []
    for species in range(2):
        molecule_weight = masses[species]
        speed_x, speed_y, speed_z, spacing = lattice(vel_order, molecule_weight)
        moment_rows, shape_rows, square = features(speed_x, speed_y, speed_z, molecule_weight)
        flat_dist = distribution[species].reshape(cell_count, NVEL)
        coeffs = coefficients(moments[species], blended_gas_mean, molecule_weight, spacing)
        collided = collide(flat_dist, coeffs, blended_gas_mean[4], shape_rows).reshape(NX, NY, NVEL)
        emitted = wall_law(square, spacing, molecule_weight)
        factor = wall_weight * incident[species] / wall_scale(molecule_weight) + inflow_weight * PORT_DENSITY
        ghost_low = factor[:, 0:1] * emitted[None, :]
        ghost_high = factor[:, 1:2] * emitted[None, :]
        left_cells = jnp.roll(collided, 1, axis=0)
        right_cells = jnp.roll(collided, -1, axis=0)
        results.append(stream(collided, left_cells, right_cells, ghost_low, ghost_high, speed_x, speed_y))
    return jnp.stack(results)
```

```python
import math

import jax
import jax.numpy as jnp
from jax import lax
from jax.experimental import pallas as pl
from jax.experimental.pallas import tpu as pltpu
from jax.sharding import PartitionSpec as P

NV = 32
NVEL = NV**3
BITS = NV.bit_length() - 1

TIME_STEP = 0.1
RAREFACTION = 0.5
PORT_DENSITY = 1.0
HALF_RANGE = 4.5
CENTRE = (NV - 1) / 2.0
STEP = 2.0 * HALF_RANGE / (NV - 1)
KAPPA = STEP * STEP
LOG2E = math.log2(math.e)

NEAR = 4
FAN = 4

F32 = jnp.float32
BF16 = jnp.bfloat16
MESH = pl.DeviceIdType.MESH


def pieces(rows):
    high = rows.astype(BF16).astype(F32)
    rest = rows - high
    middle = rest.astype(BF16).astype(F32)
    return jnp.concatenate([high, middle, rest - middle], axis=0).astype(BF16)


def lattice(order):
    index_a = lax.shift_right_logical(order, 2 * BITS).astype(F32)
    index_b = (lax.shift_right_logical(order, BITS) & (NV - 1)).astype(F32)
    index_e = (order & (NV - 1)).astype(F32)
    return index_a - CENTRE, index_b - CENTRE, index_e - CENTRE


def split_square(a, b, e):
    square = a * a + b * b + e * e
    coarse = jnp.floor(square * (1.0 / 32.0)) * 32.0
    return square, coarse, square - coarse


def rows_of(choices, shape):
    row = lax.broadcasted_iota(jnp.int32, shape, 0)
    out = choices[-1]
    for i in range(len(choices) - 2, -1, -1):
        out = jnp.where(row == i, choices[i], out)
    return out


def kernel(
    dist_in, order_in, mass_in, wall_in, inflow_in, out,
    order, mass, wall, inflow, msg, inbox, far_out, far_in, coef, halo_d, halo_c,
    w, lane, flux, coll,
    small_sem, msg_send, inbox_sem, far_send, far_recv, coef_send, coef_recv,
    halo_d_send, halo_d_recv, halo_c_send, halo_c_recv, ready,
):
    z, x, s = lax.axis_index("vel"), lax.axis_index("space"), lax.axis_index("spec")
    nz, nx = lax.axis_size("vel"), lax.axis_size("space")
    left, right = lax.rem(x + nx - 1, nx), lax.rem(x + 1, nx)
    d = dist_in.at[0]
    slab, cross, vel = d.shape
    pairs = slab // 2
    cells = slab * cross
    is_root = z == 0
    is_leader = lax.rem(z, FAN) == 0
    leader = z - lax.rem(z, FAN)

    def near(i):
        return (i <= NEAR) | (i >= nz - NEAR)

    barrier = pltpu.get_barrier_semaphore()

    def signal(sem, **where):
        pl.semaphore_signal(sem, inc=1, device_id=where, device_id_type=MESH)

    smalls = [
        pltpu.make_async_copy(order_in, order, small_sem.at[0]),
        pltpu.make_async_copy(mass_in, mass, small_sem.at[1]),
        pltpu.make_async_copy(wall_in, wall, small_sem.at[2]),
        pltpu.make_async_copy(inflow_in, inflow, small_sem.at[3]),
    ]
    for copy in smalls:
        copy.start()

    signal(barrier, space=left)
    signal(barrier, space=right)

    @pl.when(is_root)
    def _():
        signal(barrier, spec=1 - s)

        def tell(i, carry):
            @pl.when((s == 1) | near(i))
            def _():
                signal(barrier, vel=i, spec=0)
                signal(barrier, vel=i, spec=1)

            return carry

        lax.fori_loop(1, nz, tell, 0)

    @pl.when(is_leader & (z > 0))
    def _():
        for k in range(1, FAN):
            signal(barrier, vel=z + k)

    smalls[0].wait()
    smalls[1].wait()
    a, b, e = lattice(jnp.broadcast_to(order[...], (8, vel)))
    square, coarse, fine = split_square(a, b, e)
    phi = rows_of([jnp.ones_like(a), jnp.ones_like(a), a, b, e, coarse, fine, jnp.abs(b)], a.shape)
    phi = phi.astype(BF16)

    m = jnp.full((8, 128), mass[0], jnp.int32).astype(F32)
    root_m = jnp.sqrt(m)
    unit = jnp.full((8, 128), 1.0 / NVEL, F32)
    speed = root_m * (STEP / NVEL)
    energy = jnp.full((8, 128), 0.5 * KAPPA / NVEL, F32)
    scale = rows_of([unit, m * unit, speed, speed, speed, energy, energy, speed], m.shape)
    nt = (((1,), (1,)), ((), ()))
    for p in range(pairs):
        block = d[2 * p : 2 * p + 2].reshape(2 * cross, vel)
        high = block.astype(BF16)
        low = (block - high.astype(F32)).astype(BF16)
        part = lax.dot_general(phi, high, nt, preferred_element_type=F32)
        part += lax.dot_general(phi, low, nt, preferred_element_type=F32)
        msg[:, 128 * p : 128 * (p + 1)] = part * scale

    def one(flag):
        return jnp.where(flag, 1, 0)

    pl.semaphore_wait(
        barrier,
        2 + one(is_root) + one(z > 0) * (1 + one(near(z))) + one((z > FAN) & (leader != z)),
    )

    def to_root(core):
        slot = one(s != core)
        return pltpu.make_async_remote_copy(
            src_ref=msg,
            dst_ref=inbox.at[z, slot],
            send_sem=msg_send.at[core],
            recv_sem=inbox_sem.at[z, slot],
            device_id={"vel": 0, "spec": core},
            device_id_type=MESH,
        )

    def to_partner():
        return pltpu.make_async_remote_copy(
            src_ref=msg,
            dst_ref=inbox.at[0, 1],
            send_sem=msg_send.at[0],
            recv_sem=inbox_sem.at[0, 1],
            device_id={"spec": 1 - s},
            device_id_type=MESH,
        )

    @pl.when(z > 0)
    def _():
        to_root(1).start()

        @pl.when(near(z))
        def _():
            to_root(0).start()

    @pl.when(is_root)
    def _():
        to_partner().start()

    def halo_copy(src, box, sends, recvs, side):
        return pltpu.make_async_remote_copy(
            src_ref=src,
            dst_ref=box.at[side],
            send_sem=sends.at[side],
            recv_sem=recvs.at[side],
            device_id={"space": right if side == 0 else left},
            device_id_type=MESH,
        )

    halo_ds = [
        halo_copy(d.at[slab - 1], halo_d, halo_d_send, halo_d_recv, 0),
        halo_copy(d.at[0], halo_d, halo_d_send, halo_d_recv, 1),
    ]
    for copy in halo_ds:
        copy.start()

    @pl.when((z > FAN) & (leader != z))
    def _():
        signal(ready, vel=leader)

    speed_unit = (STEP / root_m)[:, :1]
    ones = jnp.ones((8, vel), F32)
    zeros = jnp.zeros((8, 128), F32)
    last = lax.broadcasted_iota(jnp.int32, (8, 128), 0)
    table = rows_of([ones, a, b, e, coarse, fine, 0.0 * ones, 0.0 * ones], ones.shape)
    keep = jnp.where(last == 6, 1.0, zeros)
    emit = jnp.where(last == 7, 1.0, zeros)
    table = jnp.concatenate([table, keep, emit], axis=1)
    w[...] = jnp.concatenate([table, table, table], axis=0).astype(BF16)
    go_x = TIME_STEP * speed_unit * jnp.abs(a)
    go_y = TIME_STEP * speed_unit * jnp.abs(b)
    law_unit = NVEL * (KAPPA / (2.0 * math.pi)) ** 1.5
    law = law_unit * jnp.exp(-0.5 * KAPPA * square)
    lane[...] = rows_of([1.0 - go_x - go_y, go_x, go_y, a, b, law, law, law], ones.shape)

    def coef_copy(target):
        return pltpu.make_async_remote_copy(
            src_ref=coef,
            dst_ref=coef,
            send_sem=coef_send.at[target],
            recv_sem=coef_recv,
            device_id={"vel": target},
            device_id_type=MESH,
        )

    @pl.when(is_root)
    def _():
        for copy in smalls[2:]:
            copy.wait()
        shape = (1, cells)
        spot = lax.broadcasted_iota(jnp.int32, shape, 1)
        wall_row = jnp.zeros(shape, F32)
        port_row = jnp.zeros(shape, F32)
        for i in range(slab):
            for side in range(2):
                here = spot == i * cross + side * (cross - 1)
                wall_row = jnp.where(here, jnp.full(shape, wall[side, i], jnp.int32).astype(F32), wall_row)
                port_row = jnp.where(here, jnp.full(shape, inflow[side, i], jnp.int32).astype(F32), port_row)
        mass_row = jnp.full(shape, mass[0], jnp.int32).astype(F32)
        point = lax.broadcasted_iota(jnp.int32, shape, 1)
        offset = point.astype(F32) - CENTRE
        bell = jnp.where(point < NV, jnp.exp(-0.5 * KAPPA * offset * offset), 0.0)
        bell_sum = jnp.sum(bell, axis=1, keepdims=True)
        flow_sum = jnp.sum(jnp.maximum(offset, 0.0) * bell, axis=1, keepdims=True)
        root_row = jnp.sqrt(mass_row)
        scale_row = (KAPPA / (2.0 * math.pi)) ** 1.5 * flow_sum * bell_sum * bell_sum
        wall_row = wall_row / (2.0 * STEP * root_row * scale_row)
        port_row = port_row * PORT_DENSITY
        sign = jnp.where(lax.rem(spot, cross) == 0, -1.0, 1.0)

        def arrive(i, slot):
            pltpu.make_async_remote_copy(
                src_ref=msg,
                dst_ref=inbox.at[i, slot],
                send_sem=msg_send.at[0],
                recv_sem=inbox_sem.at[i, slot],
                device_id={"spec": 1 - s},
                device_id_type=MESH,
            ).wait_recv()
            return inbox[i, slot]

        def take(i, carry):
            own, other = carry
            return own + arrive(i, 0), other + arrive(i, 1)

        def far_copy():
            return pltpu.make_async_remote_copy(
                src_ref=far_out,
                dst_ref=far_in,
                send_sem=far_send,
                recv_sem=far_recv,
                device_id={"spec": 1 - s},
                device_id_type=MESH,
            )

        if nz > 2 * NEAR + 1:

            @pl.when(s == 1)
            def _():
                nothing = jnp.zeros((8, cells), F32)
                own, other = lax.fori_loop(NEAR + 1, nz - NEAR, take, (nothing, nothing))
                far_out[0] = other
                far_out[1] = own
                far_in[0] = own
                far_in[1] = other
                far_copy().start()

            @pl.when(s == 0)
            def _():
                far_copy().wait_recv()

            sums = (far_in[0], far_in[1])
        else:
            sums = (jnp.zeros((8, cells), F32), jnp.zeros((8, cells), F32))
        sums = (sums[0] + msg[...], sums[1] + arrive(0, 1))
        nears = [i for i in range(1, nz) if i <= NEAR or i >= nz - NEAR]
        for i in nears:
            sums = take(i, sums)
        own, other = sums
        total = own + other

        density = total[0:1]
        per_density = 1.0 / density
        weight = total[1:2]
        per_weight = 1.0 / weight
        flow_x = total[2:3] * per_weight
        flow_y = total[3:4] * per_weight
        flow_z = total[4:5] * per_weight
        flow_square = flow_x * flow_x + flow_y * flow_y + flow_z * flow_z
        heat = 2.0 / 3.0 * (total[5:6] + total[6:7] - 0.5 * weight * flow_square) * per_density
        sharp = mass_row / heat
        pace = (TIME_STEP / RAREFACTION) * density
        spacing = STEP / root_row
        bulk = sharp * (1.0 / (2.0 * math.pi))
        height = own[0:1] * pace * (NVEL * spacing * spacing * spacing) * bulk * jnp.sqrt(bulk)
        coef[0:1] = LOG2E * (jnp.log(height) - 0.5 * sharp * flow_square)
        slope = LOG2E * sharp * spacing
        coef[1:2] = slope * flow_x
        coef[2:3] = slope * flow_y
        coef[3:4] = slope * flow_z
        curve = -0.5 * slope * spacing
        coef[4:5] = curve
        coef[5:6] = curve
        coef[6:7] = 1.0 - pace
        coef[7:8] = wall_row * (own[7:8] + sign * own[3:4]) + port_row

    @pl.when(is_root)
    def _():
        for k in range(1, min(FAN, nz)):
            coef_copy(k).start()

    @pl.when(jnp.logical_not(is_root))
    def _():
        coef_copy(0).wait_recv()

    halo_cs = [
        halo_copy(coef.at[:, pl.ds(cells - 128, 128)], halo_c, halo_c_send, halo_c_recv, 0),
        halo_copy(coef.at[:, pl.ds(0, 128)], halo_c, halo_c_send, halo_c_recv, 1),
    ]
    for copy in halo_cs:
        copy.start()

    @pl.when(is_root)
    def _():
        for k in range(FAN, nz, FAN):
            coef_copy(k).start()

    @pl.when(is_leader & (z > 0))
    def _():
        pl.semaphore_wait(ready, FAN - 1)
        for k in range(1, FAN):
            coef_copy(z + k).start()

    tn = (((0,), (0,)), ((), ()))
    width = 256

    def collide(parts, rows, put, put_flux):
        side = lax.dot_general(parts, w[:, vel : vel + 256], tn, preferred_element_type=F32)
        stay = jnp.concatenate([side[:, :128]] * (width // 128), axis=1)
        if put_flux is not None:
            put_flux(side[:, 128:].reshape(2, cross, 128))
        for c in range(0, vel, width):
            power = lax.dot_general(parts, w[:, c : c + width], tn, preferred_element_type=F32)
            old = rows(c).reshape(2 * cross, width)
            put(c, (old * stay + jnp.exp2(power)).reshape(2, cross, width))

    for p in range(pairs):

        def rows(c, p=p):
            return d[2 * p : 2 * p + 2, :, c : c + width]

        def put(c, value, p=p):
            coll[2 * p + 1 : 2 * p + 3, :, c : c + width] = value

        def put_flux(value, p=p):
            flux[2 * p : 2 * p + 2] = value

        collide(pieces(coef[:, 128 * p : 128 * (p + 1)]), rows, put, put_flux)

    level = lax.broadcasted_iota(jnp.int32, (cross, 128), 0)

    def stream(i):
        low_flux = flux[i, 0:1]
        high_flux = flux[i, cross - 1 : cross]
        for c in range(0, vel, 128):
            cols = slice(c, c + 128)
            here = coll[i + 1, :, cols]
            law = lane[5:6, cols]
            below = jnp.where(level == 0, low_flux * law, pltpu.roll(here, 1, 0))
            above = jnp.where(level == cross - 1, high_flux * law, pltpu.roll(here, cross - 1, 0))
            beside = jnp.where(lane[3:4, cols] > 0.0, coll[i, :, cols], coll[i + 2, :, cols])
            over = jnp.where(lane[4:5, cols] > 0.0, below, above)
            out[0, i, :, cols] = (
                lane[0:1, cols] * here + lane[1:2, cols] * beside + lane[2:3, cols] * over
            )

    for i in range(1, slab - 1):
        stream(i)

    for copy in halo_ds + halo_cs:
        copy.wait_recv()
    spot = lax.broadcasted_iota(jnp.int32, (8, 128), 1)
    beside = jnp.where(spot < cross, halo_c[1], halo_c[0])

    def rows(c):
        return jnp.concatenate([halo_d[1:2, :, c : c + width], halo_d[0:1, :, c : c + width]], 0)

    def put(c, value):
        coll[slab + 1, :, c : c + width] = value[0]
        coll[0, :, c : c + width] = value[1]

    collide(pieces(beside), rows, put, None)
    stream(0)
    stream(slab - 1)

    for copy in halo_ds + halo_cs:
        copy.wait_send()

    @pl.when(z > 0)
    def _():
        to_root(1).wait_send()
        for copy in smalls[2:]:
            copy.wait()

        @pl.when(near(z))
        def _():
            to_root(0).wait_send()

    @pl.when(is_root)
    def _():
        to_partner().wait_send()
        for k in [*range(1, min(FAN, nz)), *range(FAN, nz, FAN)]:
            coef_copy(k).wait_send()
        if nz > 2 * NEAR + 1:

            @pl.when(s == 1)
            def _():
                pltpu.make_async_remote_copy(
                    src_ref=far_out,
                    dst_ref=far_in,
                    send_sem=far_send,
                    recv_sem=far_recv,
                    device_id={"spec": 1 - s},
                    device_id_type=MESH,
                ).wait_send()

    @pl.when(is_leader & (z > 0))
    def _():
        for k in range(1, FAN):
            coef_copy(z + k).wait_send()


def per_device(distribution, vel_order, species_mass, wall_mask, inflow_mask):
    _, slab, cross, vel = distribution.shape
    nz = lax.axis_size("vel")
    cells = slab * cross
    hbm = pl.BlockSpec(memory_space=pltpu.HBM)
    dma = pltpu.SemaphoreType.DMA
    return pl.pallas_call(
        kernel,
        out_shape=jax.ShapeDtypeStruct(distribution.shape, F32),
        in_specs=[pl.BlockSpec(memory_space=pltpu.VMEM)] + [hbm] * 4,
        out_specs=pl.BlockSpec(memory_space=pltpu.VMEM),
        scratch_shapes=[
            pltpu.VMEM((1, vel), jnp.int32),
            pltpu.SMEM(species_mass.shape, jnp.int32),
            pltpu.SMEM((2, slab), jnp.int32),
            pltpu.SMEM((2, slab), jnp.int32),
            pltpu.VMEM((8, cells), F32),
            pltpu.VMEM((nz, 2, 8, cells), F32),
            pltpu.VMEM((2, 8, cells), F32),
            pltpu.VMEM((2, 8, cells), F32),
            pltpu.VMEM((8, cells), F32),
            pltpu.VMEM((2, cross, vel), F32),
            pltpu.VMEM((2, 8, 128), F32),
            pltpu.VMEM((24, vel + 256), BF16),
            pltpu.VMEM((8, vel), F32),
            pltpu.VMEM((slab, cross, 128), F32),
            pltpu.VMEM((slab + 2, cross, vel), F32),
            dma((4,)),
            dma((2,)),
            dma((nz, 2)),
            dma(()),
            dma(()),
            dma((nz,)),
            dma(()),
            dma((2,)),
            dma((2,)),
            dma((2,)),
            dma((2,)),
            pltpu.SemaphoreType.REGULAR,
        ],
        compiler_params=pltpu.CompilerParams(
            collective_id=0, has_side_effects=True, vmem_limit_bytes=32 * 1024 * 1024
        ),
    )(distribution, vel_order.reshape(1, vel), species_mass, wall_mask.T, inflow_mask.T)


def solution(mesh):
    in_specs = (
        P("spec", ("groups", "space"), None, "vel"),
        P("vel"),
        P("spec"),
        P(("groups", "space"), None),
        P(("groups", "space"), None),
    )
    out_specs = P("spec", ("groups", "space"), None, "vel")
    return jax.shard_map(
        per_device, mesh=mesh, in_specs=in_specs, out_specs=out_specs, check_vma=False
    )
```

```python
import math

import jax
import jax.numpy as jnp
from jax import lax
from jax.experimental import pallas as pl
from jax.experimental.pallas import tpu as pltpu
from jax.sharding import PartitionSpec as P

NV = 32
NVEL = NV**3
BITS = NV.bit_length() - 1

TIME_STEP = 0.1
RAREFACTION = 0.5
PORT_DENSITY = 1.0
HALF_RANGE = 4.5
CENTRE = (NV - 1) / 2.0
STEP = 2.0 * HALF_RANGE / (NV - 1)
KAPPA = STEP * STEP
LOG2E = math.log2(math.e)

ROOT = 1
ROWS = 6
FAN = 4

F32 = jnp.float32
BF16 = jnp.bfloat16
MESH = pl.DeviceIdType.MESH


def pieces(rows):
    high = rows.astype(BF16).astype(F32)
    rest = rows - high
    middle = rest.astype(BF16).astype(F32)
    return jnp.concatenate([high, middle, rest - middle], axis=0).astype(BF16)


def lattice(order):
    index_a = lax.shift_right_logical(order, 2 * BITS).astype(F32)
    index_b = (lax.shift_right_logical(order, BITS) & (NV - 1)).astype(F32)
    index_e = (order & (NV - 1)).astype(F32)
    return index_a - CENTRE, index_b - CENTRE, index_e - CENTRE


def split_square(a, b, e):
    square = a * a + b * b + e * e
    coarse = jnp.floor(square * (1.0 / 32.0)) * 32.0
    return square, coarse, square - coarse


def rows_of(choices, shape):
    row = lax.broadcasted_iota(jnp.int32, shape, 0)
    out = choices[-1]
    for i in range(len(choices) - 2, -1, -1):
        out = jnp.where(row == i, choices[i], out)
    return out


def kernel(
    dist_in, order_in, mass_in, wall_in, inflow_in, out,
    d, order, mass, wall, inflow, msg, inbox, coef, coef_other, halo_d, halo_c,
    w, lane, flux, coll,
    load_sem, small_sem, msg_send, inbox_sem, coef_send, coef_recv,
    halo_d_send, halo_d_recv, halo_c_send, halo_c_recv, ready,
):
    z, x, s = lax.axis_index("vel"), lax.axis_index("space"), lax.axis_index("spec")
    nz, nx = lax.axis_size("vel"), lax.axis_size("space")
    left, right = lax.rem(x + nx - 1, nx), lax.rem(x + 1, nx)
    slab, cross, vel = d.shape
    pairs = slab // 2
    is_root = (z == 0) & (s == ROOT)
    is_leader = lax.rem(z, FAN) == 0
    leader = z - lax.rem(z, FAN)

    barrier = pltpu.get_barrier_semaphore()

    def signal(sem, **where):
        pl.semaphore_signal(sem, inc=1, device_id=where, device_id_type=MESH)

    smalls = [
        pltpu.make_async_copy(order_in, order, small_sem.at[0]),
        pltpu.make_async_copy(mass_in, mass, small_sem.at[1]),
        pltpu.make_async_copy(wall_in, wall, small_sem.at[2]),
        pltpu.make_async_copy(inflow_in, inflow, small_sem.at[3]),
    ]
    loads = [
        pltpu.make_async_copy(
            dist_in.at[0, pl.ds(2 * p, 2)], d.at[pl.ds(2 * p, 2)], load_sem.at[p]
        )
        for p in range(pairs)
    ]
    for copy in smalls[:2] + loads + smalls[2:]:
        copy.start()

    signal(barrier, space=left)
    signal(barrier, space=right)

    @pl.when(is_root)
    def _():
        signal(barrier, spec=1 - s)

        def tell(i, carry):
            signal(barrier, vel=i, spec=0)
            signal(barrier, vel=i, spec=1)
            return carry

        lax.fori_loop(1, nz, tell, 0)

    @pl.when(is_leader & (z > 0))
    def _():
        for k in range(1, FAN):
            signal(barrier, vel=z + k)

    smalls[0].wait()
    smalls[1].wait()
    a, b, e = lattice(jnp.broadcast_to(order[...], (8, vel)))
    square, coarse, fine = split_square(a, b, e)
    phi = rows_of([jnp.ones_like(a), jnp.abs(b), a, b, e, coarse, fine, fine], a.shape)
    phi = phi.astype(BF16)

    m = jnp.full((8, 128), mass[0], jnp.int32).astype(F32)
    root_m = jnp.sqrt(m)
    unit = jnp.full((8, 128), 1.0 / NVEL, F32)
    speed = root_m * (STEP / NVEL)
    energy = jnp.full((8, 128), 0.5 * KAPPA / NVEL, F32)
    scale = rows_of([unit, speed, speed, speed, speed, energy, energy, energy], m.shape)
    row = lax.broadcasted_iota(jnp.int32, (8, 128), 0)
    height = lax.broadcasted_iota(jnp.int32, (8, 128), 1) % cross
    inner = (height > 0) & (height < cross - 1)
    nt = (((1,), (1,)), ((), ()))
    for p in range(pairs):
        loads[p].wait()
        block = d[2 * p : 2 * p + 2].reshape(2 * cross, vel)
        high = block.astype(BF16)
        low = (block - high.astype(F32)).astype(BF16)
        part = lax.dot_general(phi, high, nt, preferred_element_type=F32)
        part += lax.dot_general(phi, low, nt, preferred_element_type=F32)
        part = (part + jnp.where(row == 5, pltpu.roll(part, 7, 0), 0.0)) * scale
        msg[:, p, :] = jnp.where((row == 1) & inner, m, part)[:ROWS]

    def one(flag):
        return jnp.where(flag, 1, 0)

    pl.semaphore_wait(
        barrier, 2 + one(jnp.logical_not(is_root)) + one((z > FAN) & (leader != z))
    )

    def to_root():
        return pltpu.make_async_remote_copy(
            src_ref=msg,
            dst_ref=inbox.at[z, s],
            send_sem=msg_send,
            recv_sem=inbox_sem.at[z, s],
            device_id={"vel": 0, "spec": ROOT},
            device_id_type=MESH,
        )

    @pl.when(jnp.logical_not(is_root))
    def _():
        to_root().start()

    def halo_copy(src, box, sends, recvs, side):
        return pltpu.make_async_remote_copy(
            src_ref=src,
            dst_ref=box.at[side],
            send_sem=sends.at[side],
            recv_sem=recvs.at[side],
            device_id={"space": right if side == 0 else left},
            device_id_type=MESH,
        )

    halo_ds = [
        halo_copy(d.at[slab - 1], halo_d, halo_d_send, halo_d_recv, 0),
        halo_copy(d.at[0], halo_d, halo_d_send, halo_d_recv, 1),
    ]
    for copy in halo_ds:
        copy.start()

    @pl.when((z > FAN) & (leader != z))
    def _():
        signal(ready, vel=leader)

    speed_unit = (STEP / root_m)[:, :1]
    ones = jnp.ones((8, vel), F32)
    zeros = jnp.zeros((8, 128), F32)
    table = rows_of([ones, a, b, e, coarse, fine, 0.0 * ones, 0.0 * ones], ones.shape)
    keep = jnp.where(row == 6, 1.0, zeros)
    emit = jnp.where(row == 7, 1.0, zeros)
    table = jnp.concatenate([table, keep, emit], axis=1)
    w[...] = jnp.concatenate([table, table, table], axis=0).astype(BF16)
    go_x = TIME_STEP * speed_unit * jnp.abs(a)
    go_y = TIME_STEP * speed_unit * jnp.abs(b)
    law_unit = NVEL * (KAPPA / (2.0 * math.pi)) ** 1.5
    law = law_unit * jnp.exp(-0.5 * KAPPA * square)
    lane[...] = rows_of([1.0 - go_x - go_y, go_x, go_y, a, b, law, law, law], ones.shape)

    def coef_copy(i, core, own):
        return pltpu.make_async_remote_copy(
            src_ref=coef if own else coef_other,
            dst_ref=coef,
            send_sem=coef_send.at[i, core],
            recv_sem=coef_recv,
            device_id={"vel": i, "spec": core},
            device_id_type=MESH,
        )

    def served(places):
        nearest = sorted(places, key=lambda i: min(i, nz - i))
        return [coef_copy(i, core, core == ROOT) for i in nearest for core in (ROOT, 1 - ROOT)]

    beside, leaders = range(1, min(FAN, nz)), range(FAN, nz, FAN)

    @pl.when(is_root)
    def _():
        for copy in smalls[2:]:
            copy.wait()
        shape = (pairs, 128)
        spot = lax.broadcasted_iota(jnp.int32, shape, 0) * 128
        spot = spot + lax.broadcasted_iota(jnp.int32, shape, 1)
        wall_row = jnp.zeros(shape, F32)
        port_row = jnp.zeros(shape, F32)
        for i in range(slab):
            for side in range(2):
                here = spot == i * cross + side * (cross - 1)
                wall_row = jnp.where(here, jnp.full(shape, wall[side, i], jnp.int32).astype(F32), wall_row)
                port_row = jnp.where(here, jnp.full(shape, inflow[side, i], jnp.int32).astype(F32), port_row)
        port_row = port_row * PORT_DENSITY
        offset = spot.astype(F32) - CENTRE
        bell = jnp.where(spot < NV, jnp.exp(-0.5 * KAPPA * offset * offset), 0.0)
        bell_sum = jnp.sum(jnp.sum(bell, axis=1, keepdims=True), axis=0, keepdims=True)
        flow = jnp.maximum(offset, 0.0) * bell
        flow_sum = jnp.sum(jnp.sum(flow, axis=1, keepdims=True), axis=0, keepdims=True)
        sign = jnp.where(lax.rem(spot, cross) == 0, -1.0, 1.0)
        law_scale = (2.0 * STEP) * (KAPPA / (2.0 * math.pi)) ** 1.5 * flow_sum * bell_sum * bell_sum

        def arrive(i, core):
            pltpu.make_async_remote_copy(
                src_ref=msg,
                dst_ref=inbox.at[i, core],
                send_sem=msg_send,
                recv_sem=inbox_sem.at[i, core],
                device_id={"spec": 1 - s},
                device_id_type=MESH,
            ).wait_recv()
            return inbox[i, core]

        mine, partner = msg[...], arrive(0, 1 - ROOT)
        spot_b = lax.rem(spot, cross)
        between = (spot_b > 0) & (spot_b < cross - 1)
        masses = []
        for part in (mine, partner):
            found = jnp.where(between, part[1], 0.0)
            found = jnp.max(jnp.max(found, axis=1, keepdims=True), axis=0, keepdims=True)
            masses.append(jnp.broadcast_to(found, shape))
        spacings = [STEP / jnp.sqrt(v) for v in masses]
        walls = [wall_row / (jnp.sqrt(v) * law_scale) for v in masses]
        volumes = [
            (TIME_STEP / RAREFACTION) * NVEL * v * v * v * (0.5 / math.pi) for v in spacings
        ]

        def take(i, carry):
            first, second = carry
            return first + arrive(i, ROOT), second + arrive(i, 1 - ROOT)

        own, other = lax.fori_loop(1, nz, take, (mine, partner))

        density = own[0] + other[0]
        per_density = 1.0 / density
        weight = masses[0] * own[0] + masses[1] * other[0]
        per_weight = 1.0 / weight
        flow_x = (own[2] + other[2]) * per_weight
        flow_y = (own[3] + other[3]) * per_weight
        flow_z = (own[4] + other[4]) * per_weight
        flow_square = flow_x * flow_x + flow_y * flow_y + flow_z * flow_z
        heat = 2.0 / 3.0 * (own[5] + other[5] - 0.5 * weight * flow_square) * per_density
        per_heat = 1.0 / heat
        for part, v, h, wall_v, volume, box in (
            (own, masses[0], spacings[0], walls[0], volumes[0], coef),
            (other, masses[1], spacings[1], walls[1], volumes[1], coef_other),
        ):
            sharp = v * per_heat
            top = part[0] * density * volume * sharp * jnp.sqrt(sharp * (0.5 / math.pi))
            slope = LOG2E * h * sharp
            curve = -0.5 * h * slope
            rows = [
                LOG2E * (jnp.log(top) - 0.5 * sharp * flow_square),
                slope * flow_x,
                slope * flow_y,
                slope * flow_z,
                curve,
                curve,
                1.0 - (TIME_STEP / RAREFACTION) * density,
                wall_v * (part[1] + sign * part[3]) + port_row,
            ]
            for i, values in enumerate(rows):
                box[:, i, :] = values

        coef_copy(0, 1 - ROOT, False).start()

    @pl.when(jnp.logical_not(is_root))
    def _():
        coef_copy(z, s, True).wait_recv()

    halo_cs = [
        halo_copy(coef.at[pairs - 1], halo_c, halo_c_send, halo_c_recv, 0),
        halo_copy(coef.at[0], halo_c, halo_c_send, halo_c_recv, 1),
    ]
    for copy in halo_cs:
        copy.start()

    @pl.when(is_root)
    def _():
        for copy in served(beside):
            copy.start()

    def pass_on():
        return [coef_copy(z + k, s, True) for k in range(1, FAN)]

    @pl.when(is_leader & (z > 0))
    def _():
        pl.semaphore_wait(ready, FAN - 1)
        for copy in pass_on():
            copy.start()

    tn = (((0,), (0,)), ((), ()))
    width = 256

    def collide(parts, rows, put, put_flux):
        side = lax.dot_general(parts, w[:, vel : vel + 256], tn, preferred_element_type=F32)
        stay = jnp.concatenate([side[:, :128]] * (width // 128), axis=1)
        if put_flux is not None:
            put_flux(side[:, 128:].reshape(2, cross, 128))
        for c in range(0, vel, width):
            power = lax.dot_general(parts, w[:, c : c + width], tn, preferred_element_type=F32)
            old = rows(c).reshape(2 * cross, width)
            put(c, (old * stay + jnp.exp2(power)).reshape(2, cross, width))

    for p in range(pairs):

        def rows(c, p=p):
            return d[2 * p : 2 * p + 2, :, c : c + width]

        def put(c, value, p=p):
            coll[2 * p + 1 : 2 * p + 3, :, c : c + width] = value

        def put_flux(value, p=p):
            flux[2 * p : 2 * p + 2] = value

        collide(pieces(coef[p]), rows, put, put_flux)

    @pl.when(is_root)
    def _():
        for copy in served(leaders):
            copy.start()

    level = lax.broadcasted_iota(jnp.int32, (cross, 128), 0)

    def stream(i):
        low_flux = flux[i, 0:1]
        high_flux = flux[i, cross - 1 : cross]
        for c in range(0, vel, 128):
            cols = slice(c, c + 128)
            here = coll[i + 1, :, cols]
            law = lane[5:6, cols]
            below = jnp.where(level == 0, low_flux * law, pltpu.roll(here, 1, 0))
            above = jnp.where(level == cross - 1, high_flux * law, pltpu.roll(here, cross - 1, 0))
            beside = jnp.where(lane[3:4, cols] > 0.0, coll[i, :, cols], coll[i + 2, :, cols])
            over = jnp.where(lane[4:5, cols] > 0.0, below, above)
            out[0, i, :, cols] = (
                lane[0:1, cols] * here + lane[1:2, cols] * beside + lane[2:3, cols] * over
            )

    for i in range(1, slab - 1):
        stream(i)

    for copy in halo_ds + halo_cs:
        copy.wait_recv()
    spot = lax.broadcasted_iota(jnp.int32, (8, 128), 1)
    outer = jnp.where(spot < cross, halo_c[1], halo_c[0])

    def rows(c):
        return jnp.concatenate([halo_d[1:2, :, c : c + width], halo_d[0:1, :, c : c + width]], 0)

    def put(c, value):
        coll[slab + 1, :, c : c + width] = value[0]
        coll[0, :, c : c + width] = value[1]

    collide(pieces(outer), rows, put, None)
    stream(0)
    stream(slab - 1)

    for copy in halo_ds + halo_cs:
        copy.wait_send()

    @pl.when(jnp.logical_not(is_root))
    def _():
        to_root().wait_send()
        for copy in smalls[2:]:
            copy.wait()

    @pl.when(is_root)
    def _():
        coef_copy(0, 1 - ROOT, False).wait_send()
        for copy in served(beside) + served(leaders):
            copy.wait_send()

    @pl.when(is_leader & (z > 0))
    def _():
        for copy in pass_on():
            copy.wait_send()


def per_device(distribution, vel_order, species_mass, wall_mask, inflow_mask):
    _, slab, cross, vel = distribution.shape
    nz = lax.axis_size("vel")
    pairs = slab // 2
    hbm = pl.BlockSpec(memory_space=pltpu.HBM)

    def stay(array):
        return pltpu.with_memory_space_constraint(array, pltpu.HBM)

    dma = pltpu.SemaphoreType.DMA
    return pl.pallas_call(
        kernel,
        out_shape=jax.ShapeDtypeStruct(distribution.shape, F32),
        in_specs=[hbm] * 5,
        out_specs=pl.BlockSpec(memory_space=pltpu.VMEM),
        scratch_shapes=[
            pltpu.VMEM((slab, cross, vel), F32),
            pltpu.VMEM((1, vel), jnp.int32),
            pltpu.SMEM(species_mass.shape, jnp.int32),
            pltpu.SMEM((2, slab), jnp.int32),
            pltpu.SMEM((2, slab), jnp.int32),
            pltpu.VMEM((ROWS, pairs, 128), F32),
            pltpu.VMEM((nz, 2, ROWS, pairs, 128), F32),
            pltpu.VMEM((pairs, 8, 128), F32),
            pltpu.VMEM((pairs, 8, 128), F32),
            pltpu.VMEM((2, cross, vel), F32),
            pltpu.VMEM((2, 8, 128), F32),
            pltpu.VMEM((24, vel + 256), BF16),
            pltpu.VMEM((8, vel), F32),
            pltpu.VMEM((slab, cross, 128), F32),
            pltpu.VMEM((slab + 2, cross, vel), F32),
            dma((slab // 2,)),
            dma((4,)),
            dma(()),
            dma((nz, 2)),
            dma((nz, 2)),
            dma(()),
            dma((2,)),
            dma((2,)),
            dma((2,)),
            dma((2,)),
            pltpu.SemaphoreType.REGULAR,
        ],
        compiler_params=pltpu.CompilerParams(
            collective_id=0, has_side_effects=True, vmem_limit_bytes=32 * 1024 * 1024
        ),
    )(
        stay(distribution),
        stay(vel_order.reshape(1, vel)),
        species_mass,
        stay(wall_mask.T),
        stay(inflow_mask.T),
    )


def solution(mesh):
    in_specs = (
        P("spec", ("groups", "space"), None, "vel"),
        P("vel"),
        P("spec"),
        P(("groups", "space"), None),
        P(("groups", "space"), None),
    )
    out_specs = P("spec", ("groups", "space"), None, "vel")
    return jax.shard_map(
        per_device, mesh=mesh, in_specs=in_specs, out_specs=out_specs, check_vma=False
    )
```

```python
import math

import jax
import jax.numpy as jnp
from jax import lax
from jax.experimental import pallas as pl
from jax.experimental.pallas import tpu as pltpu
from jax.sharding import PartitionSpec as P

NV = 32
NVEL = NV**3
BITS = NV.bit_length() - 1

TIME_STEP = 0.1
RAREFACTION = 0.5
PORT_DENSITY = 1.0
HALF_RANGE = 4.5
CENTRE = (NV - 1) / 2.0
STEP = 2.0 * HALF_RANGE / (NV - 1)
KAPPA = STEP * STEP
LOG2E = math.log2(math.e)

ROOT = 1
ROWS = 6
DETOUR = 3
FAN = 4

F32 = jnp.float32
BF16 = jnp.bfloat16
MESH = pl.DeviceIdType.MESH


def pieces(rows):
    high = rows.astype(BF16).astype(F32)
    rest = rows - high
    middle = rest.astype(BF16).astype(F32)
    return jnp.concatenate([high, middle, rest - middle], axis=0).astype(BF16)


def lattice(order):
    index_a = lax.shift_right_logical(order, 2 * BITS).astype(F32)
    index_b = (lax.shift_right_logical(order, BITS) & (NV - 1)).astype(F32)
    index_e = (order & (NV - 1)).astype(F32)
    return index_a - CENTRE, index_b - CENTRE, index_e - CENTRE


def split_square(a, b, e):
    square = a * a + b * b + e * e
    coarse = jnp.floor(square * (1.0 / 32.0)) * 32.0
    return square, coarse, square - coarse


def rows_of(choices, shape):
    row = lax.broadcasted_iota(jnp.int32, shape, 0)
    out = choices[-1]
    for i in range(len(choices) - 2, -1, -1):
        out = jnp.where(row == i, choices[i], out)
    return out


def kernel(
    dist_in, order_in, mass_in, wall_in, inflow_in, out,
    d, order, mass, wall, inflow, msg, inbox, relay, coef, coef_other, halo_d, halo_c,
    w, lane, flux, coll,
    load_sem, small_sem, msg_send, inbox_sem, relay_sem, coef_send, coef_recv,
    halo_d_send, halo_d_recv, halo_c_send, halo_c_recv, halo_r_send, ready,
):
    z, x, s = lax.axis_index("vel"), lax.axis_index("space"), lax.axis_index("spec")
    nz, nx = lax.axis_size("vel"), lax.axis_size("space")
    left, right = lax.rem(x + nx - 1, nx), lax.rem(x + 1, nx)
    slab, cross, vel = d.shape
    pairs = slab // 2
    is_root = (z == 0) & (s == ROOT)
    is_leader = lax.rem(z, FAN) == 0
    leader = z - lax.rem(z, FAN)
    middle = nz // 2 - 1
    is_middle = z == middle
    by_middle = (z > middle) & (z <= middle + DETOUR)
    is_first = z < FAN

    barrier = pltpu.get_barrier_semaphore()

    def signal(sem, **where):
        pl.semaphore_signal(sem, inc=1, device_id=where, device_id_type=MESH)

    smalls = [
        pltpu.make_async_copy(order_in, order, small_sem.at[0]),
        pltpu.make_async_copy(mass_in, mass, small_sem.at[1]),
        pltpu.make_async_copy(wall_in, wall, small_sem.at[2]),
        pltpu.make_async_copy(inflow_in, inflow, small_sem.at[3]),
    ]
    loads = [
        pltpu.make_async_copy(
            dist_in.at[0, pl.ds(2 * p, 2)], d.at[pl.ds(2 * p, 2)], load_sem.at[p]
        )
        for p in range(pairs)
    ]
    for copy in smalls[:2] + loads + smalls[2:]:
        copy.start()

    signal(barrier, space=left)
    signal(barrier, space=right)

    @pl.when(is_root)
    def _():
        signal(barrier, spec=1 - s)

        def tell(i, carry):
            signal(barrier, vel=i, spec=0)
            signal(barrier, vel=i, spec=1)
            return carry

        lax.fori_loop(1, middle + 1, tell, 0)
        lax.fori_loop(middle + DETOUR + 1, nz, tell, 0)

    @pl.when(is_middle)
    def _():
        for k in range(1, DETOUR + 1):
            signal(barrier, vel=z + k)

    @pl.when(is_first)
    def _():
        signal(barrier, space=left, vel=0, spec=ROOT)
        signal(barrier, space=right, vel=0, spec=ROOT)

    @pl.when(is_leader & (z > 0))
    def _():
        for k in range(1, FAN):
            signal(barrier, vel=z + k)

    smalls[0].wait()
    smalls[1].wait()
    a, b, e = lattice(jnp.broadcast_to(order[...], (8, vel)))
    square, coarse, fine = split_square(a, b, e)
    phi = rows_of([jnp.ones_like(a), jnp.abs(b), a, b, e, coarse, fine, fine], a.shape)
    phi = phi.astype(BF16)

    m = jnp.full((8, 128), mass[0], jnp.int32).astype(F32)
    root_m = jnp.sqrt(m)
    unit = jnp.full((8, 128), 1.0 / NVEL, F32)
    speed = root_m * (STEP / NVEL)
    energy = jnp.full((8, 128), 0.5 * KAPPA / NVEL, F32)
    scale = rows_of([unit, speed, speed, speed, speed, energy, energy, energy], m.shape)
    row = lax.broadcasted_iota(jnp.int32, (8, 128), 0)
    height = lax.broadcasted_iota(jnp.int32, (8, 128), 1) % cross
    inner = (height > 0) & (height < cross - 1)
    nt = (((1,), (1,)), ((), ()))
    for p in range(pairs):
        loads[p].wait()
        block = d[2 * p : 2 * p + 2].reshape(2 * cross, vel)
        high = block.astype(BF16)
        low = (block - high.astype(F32)).astype(BF16)
        part = lax.dot_general(high, phi, nt, preferred_element_type=F32)
        part += lax.dot_general(low, phi, nt, preferred_element_type=F32)
        part = part.T
        part = (part + jnp.where(row == 5, pltpu.roll(part, 7, 0), 0.0)) * scale
        msg[:, p, :] = jnp.where((row == 1) & inner, m, part)[:ROWS]

    def one(flag):
        return jnp.where(flag, 1, 0)

    pl.semaphore_wait(
        barrier,
        2 + one(jnp.logical_not(is_root)) + one((z > FAN) & (leader != z)) + 4 * FAN * one(is_root),
    )

    def to_root():
        return pltpu.make_async_remote_copy(
            src_ref=msg,
            dst_ref=inbox.at[z, s],
            send_sem=msg_send,
            recv_sem=inbox_sem.at[z, s],
            device_id={"vel": 0, "spec": ROOT},
            device_id_type=MESH,
        )

    def to_middle(i):
        return pltpu.make_async_remote_copy(
            src_ref=msg,
            dst_ref=relay.at[i],
            send_sem=msg_send,
            recv_sem=relay_sem.at[i],
            device_id={"vel": middle},
            device_id_type=MESH,
        )

    @pl.when(jnp.logical_not(is_root | by_middle | is_middle))
    def _():
        to_root().start()

    @pl.when(by_middle)
    def _():
        to_middle(z - middle - 1).start()

    def halo_copy(src, box, sends, recvs, side):
        return pltpu.make_async_remote_copy(
            src_ref=src,
            dst_ref=box.at[side],
            send_sem=sends.at[side],
            recv_sem=recvs.at[side],
            device_id={"space": right if side == 0 else left},
            device_id_type=MESH,
        )

    halo_ds = [
        halo_copy(d.at[slab - 1], halo_d, halo_d_send, halo_d_recv, 0),
        halo_copy(d.at[0], halo_d, halo_d_send, halo_d_recv, 1),
    ]
    for copy in halo_ds:
        copy.start()

    @pl.when((z > FAN) & (leader != z))
    def _():
        signal(ready, vel=leader)

    @pl.when(is_middle)
    def _():
        gathered = msg[...]
        for k in range(DETOUR):
            to_middle(k).wait_recv()
            gathered += relay[k]
        msg[...] = gathered
        to_root().start()

    speed_unit = (STEP / root_m)[:, :1]
    ones = jnp.ones((8, vel), F32)
    zeros = jnp.zeros((8, 128), F32)
    table = rows_of([ones, a, b, e, coarse, fine, 0.0 * ones, 0.0 * ones], ones.shape)
    keep = jnp.where(row == 6, 1.0, zeros)
    emit = jnp.where(row == 7, 1.0, zeros)
    table = jnp.concatenate([table, keep, emit], axis=1)
    w[...] = jnp.concatenate([table, table, table], axis=0).astype(BF16)
    go_x = TIME_STEP * speed_unit * jnp.abs(a)
    go_y = TIME_STEP * speed_unit * jnp.abs(b)
    law_unit = NVEL * (KAPPA / (2.0 * math.pi)) ** 1.5
    law = law_unit * jnp.exp(-0.5 * KAPPA * square)
    lane[...] = rows_of([1.0 - go_x - go_y, go_x, go_y, a, b, law, law, law], ones.shape)

    def coef_copy(i, core, own):
        return pltpu.make_async_remote_copy(
            src_ref=coef if own else coef_other,
            dst_ref=coef,
            send_sem=coef_send.at[i, core],
            recv_sem=coef_recv,
            device_id={"vel": i, "spec": core},
            device_id_type=MESH,
        )

    def served(places):
        nearest = sorted(places, key=lambda i: min(i, nz - i))
        return [coef_copy(i, core, core == ROOT) for i in nearest for core in (ROOT, 1 - ROOT)]

    first, others, leaders = range(1, 2), range(2, FAN), range(FAN, nz, FAN)

    def borders(places):
        return [
            pltpu.make_async_remote_copy(
                src_ref=(coef if core == ROOT else coef_other).at[pairs - 1 if side == 0 else 0],
                dst_ref=halo_c.at[side],
                send_sem=halo_r_send.at[i, core, side],
                recv_sem=halo_c_recv.at[side],
                device_id={"space": right if side == 0 else left, "vel": i, "spec": core},
                device_id_type=MESH,
            )
            for i in places
            for core in (ROOT, 1 - ROOT)
            for side in range(2)
        ]


    @pl.when(is_root)
    def _():
        for copy in smalls[2:]:
            copy.wait()
        shape = (pairs, 128)
        spot = lax.broadcasted_iota(jnp.int32, shape, 0) * 128
        spot = spot + lax.broadcasted_iota(jnp.int32, shape, 1)
        wall_row = jnp.zeros(shape, F32)
        port_row = jnp.zeros(shape, F32)
        for i in range(slab):
            for side in range(2):
                here = spot == i * cross + side * (cross - 1)
                wall_row = jnp.where(here, jnp.full(shape, wall[side, i], jnp.int32).astype(F32), wall_row)
                port_row = jnp.where(here, jnp.full(shape, inflow[side, i], jnp.int32).astype(F32), port_row)
        port_row = port_row * PORT_DENSITY
        offset = spot.astype(F32) - CENTRE
        bell = jnp.where(spot < NV, jnp.exp(-0.5 * KAPPA * offset * offset), 0.0)
        bell_sum = jnp.sum(jnp.sum(bell, axis=1, keepdims=True), axis=0, keepdims=True)
        flow = jnp.maximum(offset, 0.0) * bell
        flow_sum = jnp.sum(jnp.sum(flow, axis=1, keepdims=True), axis=0, keepdims=True)
        sign = jnp.where(lax.rem(spot, cross) == 0, -1.0, 1.0)
        law_scale = (2.0 * STEP) * (KAPPA / (2.0 * math.pi)) ** 1.5 * flow_sum * bell_sum * bell_sum

        def arrive(i, core):
            pltpu.make_async_remote_copy(
                src_ref=msg,
                dst_ref=inbox.at[i, core],
                send_sem=msg_send,
                recv_sem=inbox_sem.at[i, core],
                device_id={"spec": 1 - s},
                device_id_type=MESH,
            ).wait_recv()
            return inbox[i, core]

        mine, partner = msg[...], arrive(0, 1 - ROOT)
        spot_b = lax.rem(spot, cross)
        between = (spot_b > 0) & (spot_b < cross - 1)
        masses = []
        for part in (mine, partner):
            found = jnp.where(between, part[1], 0.0)
            found = jnp.max(jnp.max(found, axis=1, keepdims=True), axis=0, keepdims=True)
            masses.append(jnp.broadcast_to(found, shape))
        spacings = [STEP / jnp.sqrt(v) for v in masses]
        walls = [wall_row / (jnp.sqrt(v) * law_scale) for v in masses]
        volumes = [
            (TIME_STEP / RAREFACTION) * NVEL * v * v * v * (0.5 / math.pi) for v in spacings
        ]

        def take(i, carry):
            first, second = carry
            return first + arrive(i, ROOT), second + arrive(i, 1 - ROOT)

        sums = lax.fori_loop(1, middle + 1, take, (mine, partner))
        own, other = lax.fori_loop(middle + DETOUR + 1, nz, take, sums)

        density = own[0] + other[0]
        per_density = 1.0 / density
        weight = masses[0] * own[0] + masses[1] * other[0]
        per_weight = 1.0 / weight
        flow_x = (own[2] + other[2]) * per_weight
        flow_y = (own[3] + other[3]) * per_weight
        flow_z = (own[4] + other[4]) * per_weight
        flow_square = flow_x * flow_x + flow_y * flow_y + flow_z * flow_z
        heat = 2.0 / 3.0 * (own[5] + other[5] - 0.5 * weight * flow_square) * per_density
        per_heat = 1.0 / heat
        for part, v, h, wall_v, volume, box in (
            (own, masses[0], spacings[0], walls[0], volumes[0], coef),
            (other, masses[1], spacings[1], walls[1], volumes[1], coef_other),
        ):
            sharp = v * per_heat
            top = part[0] * density * volume * sharp * jnp.sqrt(sharp * (0.5 / math.pi))
            slope = LOG2E * h * sharp
            curve = -0.5 * h * slope
            rows = [
                LOG2E * (jnp.log(top) - 0.5 * sharp * flow_square),
                slope * flow_x,
                slope * flow_y,
                slope * flow_z,
                curve,
                curve,
                1.0 - (TIME_STEP / RAREFACTION) * density,
                wall_v * (part[1] + sign * part[3]) + port_row,
            ]
            for i, values in enumerate(rows):
                box[:, i, :] = values

        coef_copy(0, 1 - ROOT, False).start()
        for copy in borders(range(1)) + served(first) + borders(first):
            copy.start()

    @pl.when(jnp.logical_not(is_root))
    def _():
        coef_copy(z, s, True).wait_recv()

    halo_cs = [
        halo_copy(coef.at[pairs - 1], halo_c, halo_c_send, halo_c_recv, 0),
        halo_copy(coef.at[0], halo_c, halo_c_send, halo_c_recv, 1),
    ]

    @pl.when(jnp.logical_not(is_first))
    def _():
        for copy in halo_cs:
            copy.start()

    def pass_on():
        return [coef_copy(z + k, s, True) for k in range(1, FAN)]

    @pl.when(is_leader & (z > 0))
    def _():
        pl.semaphore_wait(ready, FAN - 1)
        for copy in pass_on():
            copy.start()

    tn = (((0,), (0,)), ((), ()))
    width = 256

    def collide(parts, rows, put, put_flux):
        side = lax.dot_general(parts, w[:, vel : vel + 256], tn, preferred_element_type=F32)
        stay = jnp.concatenate([side[:, :128]] * (width // 128), axis=1)
        if put_flux is not None:
            put_flux(side[:, 128:].reshape(2, cross, 128))
        for c in range(0, vel, width):
            power = lax.dot_general(parts, w[:, c : c + width], tn, preferred_element_type=F32)
            old = rows(c).reshape(2 * cross, width)
            put(c, (old * stay + jnp.exp2(power)).reshape(2, cross, width))

    for p in range(pairs):

        def rows(c, p=p):
            return d[2 * p : 2 * p + 2, :, c : c + width]

        def put(c, value, p=p):
            coll[2 * p + 1 : 2 * p + 3, :, c : c + width] = value

        def put_flux(value, p=p):
            flux[2 * p : 2 * p + 2] = value

        collide(pieces(coef[p]), rows, put, put_flux)

    @pl.when(is_root)
    def _():
        for copy in served(others) + borders(others) + served(leaders):
            copy.start()

    level = lax.broadcasted_iota(jnp.int32, (cross, 128), 0)

    def stream(i):
        low_flux = flux[i, 0:1]
        high_flux = flux[i, cross - 1 : cross]
        for c in range(0, vel, 128):
            cols = slice(c, c + 128)
            here = coll[i + 1, :, cols]
            law = lane[5:6, cols]
            below = jnp.where(level == 0, low_flux * law, pltpu.roll(here, 1, 0))
            above = jnp.where(level == cross - 1, high_flux * law, pltpu.roll(here, cross - 1, 0))
            beside = jnp.where(lane[3:4, cols] > 0.0, coll[i, :, cols], coll[i + 2, :, cols])
            over = jnp.where(lane[4:5, cols] > 0.0, below, above)
            out[0, i, :, cols] = (
                lane[0:1, cols] * here + lane[1:2, cols] * beside + lane[2:3, cols] * over
            )

    for i in range(1, slab - 1):
        stream(i)

    for copy in halo_ds + halo_cs:
        copy.wait_recv()
    spot = lax.broadcasted_iota(jnp.int32, (8, 128), 1)
    outer = jnp.where(spot < cross, halo_c[1], halo_c[0])

    def rows(c):
        return jnp.concatenate([halo_d[1:2, :, c : c + width], halo_d[0:1, :, c : c + width]], 0)

    def put(c, value):
        coll[slab + 1, :, c : c + width] = value[0]
        coll[0, :, c : c + width] = value[1]

    collide(pieces(outer), rows, put, None)
    stream(0)
    stream(slab - 1)

    for copy in halo_ds:
        copy.wait_send()

    @pl.when(jnp.logical_not(is_first))
    def _():
        for copy in halo_cs:
            copy.wait_send()

    @pl.when(by_middle)
    def _():
        to_middle(z - middle - 1).wait_send()

    @pl.when(jnp.logical_not(is_root | by_middle))
    def _():
        to_root().wait_send()

    @pl.when(jnp.logical_not(is_root))
    def _():
        for copy in smalls[2:]:
            copy.wait()

    @pl.when(is_root)
    def _():
        coef_copy(0, 1 - ROOT, False).wait_send()
        for copy in served([*first, *others, *leaders]) + borders(range(FAN)):
            copy.wait_send()

    @pl.when(is_leader & (z > 0))
    def _():
        for copy in pass_on():
            copy.wait_send()


def per_device(distribution, vel_order, species_mass, wall_mask, inflow_mask):
    _, slab, cross, vel = distribution.shape
    nz = lax.axis_size("vel")
    pairs = slab // 2
    hbm = pl.BlockSpec(memory_space=pltpu.HBM)

    def stay(array):
        return pltpu.with_memory_space_constraint(array, pltpu.HBM)

    dma = pltpu.SemaphoreType.DMA
    return pl.pallas_call(
        kernel,
        out_shape=jax.ShapeDtypeStruct(distribution.shape, F32),
        in_specs=[hbm] * 5,
        out_specs=pl.BlockSpec(memory_space=pltpu.VMEM),
        scratch_shapes=[
            pltpu.VMEM((slab, cross, vel), F32),
            pltpu.VMEM((1, vel), jnp.int32),
            pltpu.SMEM(species_mass.shape, jnp.int32),
            pltpu.SMEM((2, slab), jnp.int32),
            pltpu.SMEM((2, slab), jnp.int32),
            pltpu.VMEM((ROWS, pairs, 128), F32),
            pltpu.VMEM((nz, 2, ROWS, pairs, 128), F32),
            pltpu.VMEM((DETOUR, ROWS, pairs, 128), F32),
            pltpu.VMEM((pairs, 8, 128), F32),
            pltpu.VMEM((pairs, 8, 128), F32),
            pltpu.VMEM((2, cross, vel), F32),
            pltpu.VMEM((2, 8, 128), F32),
            pltpu.VMEM((24, vel + 256), BF16),
            pltpu.VMEM((8, vel), F32),
            pltpu.VMEM((slab, cross, 128), F32),
            pltpu.VMEM((slab + 2, cross, vel), F32),
            dma((slab // 2,)),
            dma((4,)),
            dma(()),
            dma((nz, 2)),
            dma((DETOUR,)),
            dma((nz, 2)),
            dma(()),
            dma((2,)),
            dma((2,)),
            dma((2,)),
            dma((2,)),
            dma((FAN, 2, 2)),
            pltpu.SemaphoreType.REGULAR,
        ],
        compiler_params=pltpu.CompilerParams(
            collective_id=0, has_side_effects=True, vmem_limit_bytes=32 * 1024 * 1024
        ),
    )(
        stay(distribution),
        stay(vel_order.reshape(1, vel)),
        species_mass,
        stay(wall_mask.T),
        stay(inflow_mask.T),
    )


def solution(mesh):
    in_specs = (
        P("spec", ("groups", "space"), None, "vel"),
        P("vel"),
        P("spec"),
        P(("groups", "space"), None),
        P(("groups", "space"), None),
    )
    out_specs = P("spec", ("groups", "space"), None, "vel")
    return jax.shard_map(
        per_device, mesh=mesh, in_specs=in_specs, out_specs=out_specs, check_vma=False
    )
```

```python
import math

import jax
import jax.numpy as jnp
from jax import lax
from jax.experimental import pallas as pl
from jax.experimental.pallas import tpu as pltpu
from jax.sharding import PartitionSpec as P

NV = 32
NVEL = NV**3
BITS = NV.bit_length() - 1

TIME_STEP = 0.1
RAREFACTION = 0.5
PORT_DENSITY = 1.0
HALF_RANGE = 4.5
CENTRE = (NV - 1) / 2.0
STEP = 2.0 * HALF_RANGE / (NV - 1)
KAPPA = STEP * STEP
LOG2E = math.log2(math.e)

ROOT = 1
ROWS = 6
LOADS = 8
FAN = 4

F32 = jnp.float32
BF16 = jnp.bfloat16
MESH = pl.DeviceIdType.MESH


def pieces(rows):
    high = rows.astype(BF16).astype(F32)
    rest = rows - high
    middle = rest.astype(BF16).astype(F32)
    return jnp.concatenate([high, middle, rest - middle], axis=0).astype(BF16)


def lattice(order):
    index_a = lax.shift_right_logical(order, 2 * BITS).astype(F32)
    index_b = (lax.shift_right_logical(order, BITS) & (NV - 1)).astype(F32)
    index_e = (order & (NV - 1)).astype(F32)
    return index_a - CENTRE, index_b - CENTRE, index_e - CENTRE


def split_square(a, b, e):
    square = a * a + b * b + e * e
    coarse = jnp.floor(square * (1.0 / 32.0)) * 32.0
    return square, coarse, square - coarse


def rows_of(choices, shape):
    row = lax.broadcasted_iota(jnp.int32, shape, 0)
    out = choices[-1]
    for i in range(len(choices) - 2, -1, -1):
        out = jnp.where(row == i, choices[i], out)
    return out


def kernel(
    dist_in, order_in, mass_in, wall_in, inflow_in, out,
    d, order, mass, wall, inflow, msg, inbox, coef, coef_other, halo_d, halo_c,
    w, lane, flux, coll,
    load_sem, small_sem, msg_send, inbox_sem, coef_send, coef_recv, pass_send,
    halo_d_send, halo_d_recv, halo_c_send, halo_c_recv, halo_r_send, ready,
):
    z, x, s = lax.axis_index("vel"), lax.axis_index("space"), lax.axis_index("spec")
    nz, nx = lax.axis_size("vel"), lax.axis_size("space")
    left, right = lax.rem(x + nx - 1, nx), lax.rem(x + 1, nx)
    slab, cross, vel = d.shape
    pairs = slab // 2
    is_root = (z == 0) & (s == ROOT)
    is_leader = lax.rem(z, FAN) == 0
    leader = z - lax.rem(z, FAN)
    middle = nz // 2 - 1
    is_first = z < FAN

    barrier = pltpu.get_barrier_semaphore()

    def signal(sem, **where):
        pl.semaphore_signal(sem, inc=1, device_id=where, device_id_type=MESH)

    def settle(ref, sem):
        pltpu.make_async_copy(ref, ref, sem).wait()

    smalls = [
        pltpu.make_async_copy(order_in, order, small_sem.at[0]),
        pltpu.make_async_copy(mass_in, mass, small_sem.at[1]),
        pltpu.make_async_copy(wall_in, wall, small_sem.at[2]),
        pltpu.make_async_copy(inflow_in, inflow, small_sem.at[3]),
    ]
    loads = [
        pltpu.make_async_copy(
            dist_in.at[0, pl.ds(i, slab // LOADS)], d.at[pl.ds(i, slab // LOADS)], load_sem
        )
        for i in range(0, slab, slab // LOADS)
    ]
    for copy in smalls[:2] + loads + smalls[2:]:
        copy.start()

    signal(barrier, space=left)
    signal(barrier, space=right)

    @pl.when(is_root)
    def _():
        signal(barrier, spec=1 - s)

        def tell(i, carry):
            signal(barrier, vel=i, spec=0)
            signal(barrier, vel=i, spec=1)
            return carry

        lax.fori_loop(1, nz, tell, 0)

    @pl.when(is_first)
    def _():
        signal(barrier, space=left, vel=0, spec=ROOT)
        signal(barrier, space=right, vel=0, spec=ROOT)

    @pl.when(is_leader & (z > 0))
    def _():
        for k in range(1, FAN):
            signal(barrier, vel=z + k)

    smalls[0].wait()
    smalls[1].wait()
    a, b, e = lattice(jnp.broadcast_to(order[...], (8, vel)))
    square, coarse, fine = split_square(a, b, e)
    phi = rows_of([jnp.ones_like(a), jnp.abs(b), a, b, e, coarse, fine, fine], a.shape)
    phi = phi.astype(BF16)

    m = jnp.full((8, 128), mass[0], jnp.int32).astype(F32)
    root_m = jnp.sqrt(m)
    unit = jnp.full((8, 128), 1.0 / NVEL, F32)
    speed = root_m * (STEP / NVEL)
    energy = jnp.full((8, 128), 0.5 * KAPPA / NVEL, F32)
    scale = rows_of([unit, speed, speed, speed, speed, energy, energy, energy], m.shape)
    row = lax.broadcasted_iota(jnp.int32, (8, 128), 0)
    height = lax.broadcasted_iota(jnp.int32, (8, 128), 1) % cross
    inner = (height > 0) & (height < cross - 1)
    nt = (((1,), (1,)), ((), ()))
    settle(d, load_sem)
    for p in range(pairs):
        block = d[2 * p : 2 * p + 2].reshape(2 * cross, vel)
        high = block.astype(BF16)
        low = (block - high.astype(F32)).astype(BF16)
        part = lax.dot_general(phi, high, nt, preferred_element_type=F32)
        part += lax.dot_general(phi, low, nt, preferred_element_type=F32)
        part = (part + jnp.where(row == 5, pltpu.roll(part, 7, 0), 0.0)) * scale
        msg[:, p, :] = jnp.where((row == 1) & inner, m, part)[:ROWS]

    def one(flag):
        return jnp.where(flag, 1, 0)

    pl.semaphore_wait(
        barrier,
        2 + one(jnp.logical_not(is_root)) + one((z > FAN) & (leader != z)) + 4 * FAN * one(is_root),
    )

    def to_root():
        return pltpu.make_async_remote_copy(
            src_ref=msg,
            dst_ref=inbox.at[z, s],
            send_sem=msg_send,
            recv_sem=inbox_sem.at[one(z > 0) + one(z > middle)],
            device_id={"vel": 0, "spec": ROOT},
            device_id_type=MESH,
        )

    @pl.when(jnp.logical_not(is_root))
    def _():
        to_root().start()

    def halo_copy(src, box, sends, recvs, side):
        return pltpu.make_async_remote_copy(
            src_ref=src,
            dst_ref=box.at[side],
            send_sem=sends,
            recv_sem=recvs,
            device_id={"space": right if side == 0 else left},
            device_id_type=MESH,
        )

    halo_ds = [
        halo_copy(d.at[slab - 1], halo_d, halo_d_send, halo_d_recv, 0),
        halo_copy(d.at[0], halo_d, halo_d_send, halo_d_recv, 1),
    ]
    for copy in halo_ds:
        copy.start()

    @pl.when((z > FAN) & (leader != z))
    def _():
        signal(ready, vel=leader)

    speed_unit = (STEP / root_m)[:, :1]
    ones = jnp.ones((8, vel), F32)
    zeros = jnp.zeros((8, 128), F32)
    table = rows_of([ones, a, b, e, coarse, fine, 0.0 * ones, 0.0 * ones], ones.shape)
    keep = jnp.where(row == 6, 1.0, zeros)
    emit = jnp.where(row == 7, 1.0, zeros)
    table = jnp.concatenate([table, keep, emit], axis=1)
    w[...] = jnp.concatenate([table, table, table], axis=0).astype(BF16)
    go_x = TIME_STEP * speed_unit * jnp.abs(a)
    go_y = TIME_STEP * speed_unit * jnp.abs(b)
    law_unit = NVEL * (KAPPA / (2.0 * math.pi)) ** 1.5
    law = law_unit * jnp.exp(-0.5 * KAPPA * square)
    lane[...] = rows_of([1.0 - go_x - go_y, go_x, go_y, a, b, law, law, law], ones.shape)

    def coef_copy(i, core, own, sem):
        return pltpu.make_async_remote_copy(
            src_ref=coef if own else coef_other,
            dst_ref=coef,
            send_sem=sem,
            recv_sem=coef_recv,
            device_id={"vel": i, "spec": core},
            device_id_type=MESH,
        )

    def served(places, sem):
        nearest = sorted(places, key=lambda i: min(i, nz - i))
        return [coef_copy(i, core, core == ROOT, sem) for i in nearest for core in (ROOT, 1 - ROOT)]

    first, others, leaders = range(1, 2), range(2, FAN), range(FAN, nz, FAN)

    def borders(places):
        return [
            pltpu.make_async_remote_copy(
                src_ref=(coef if core == ROOT else coef_other).at[pairs - 1 if side == 0 else 0],
                dst_ref=halo_c.at[side],
                send_sem=halo_r_send,
                recv_sem=halo_c_recv,
                device_id={"space": right if side == 0 else left, "vel": i, "spec": core},
                device_id_type=MESH,
            )
            for i in places
            for core in (ROOT, 1 - ROOT)
            for side in range(2)
        ]


    @pl.when(is_root)
    def _():
        for copy in smalls[2:]:
            copy.wait()
        shape = (pairs, 128)
        spot = lax.broadcasted_iota(jnp.int32, shape, 0) * 128
        spot = spot + lax.broadcasted_iota(jnp.int32, shape, 1)
        wall_row = jnp.zeros(shape, F32)
        port_row = jnp.zeros(shape, F32)
        for i in range(slab):
            for side in range(2):
                here = spot == i * cross + side * (cross - 1)
                wall_row = jnp.where(here, jnp.full(shape, wall[side, i], jnp.int32).astype(F32), wall_row)
                port_row = jnp.where(here, jnp.full(shape, inflow[side, i], jnp.int32).astype(F32), port_row)
        port_row = port_row * PORT_DENSITY
        offset = spot.astype(F32) - CENTRE
        bell = jnp.where(spot < NV, jnp.exp(-0.5 * KAPPA * offset * offset), 0.0)
        bell_sum = jnp.sum(jnp.sum(bell, axis=1, keepdims=True), axis=0, keepdims=True)
        flow = jnp.maximum(offset, 0.0) * bell
        flow_sum = jnp.sum(jnp.sum(flow, axis=1, keepdims=True), axis=0, keepdims=True)
        sign = jnp.where(lax.rem(spot, cross) == 0, -1.0, 1.0)
        law_scale = (2.0 * STEP) * (KAPPA / (2.0 * math.pi)) ** 1.5 * flow_sum * bell_sum * bell_sum

        settle(inbox.at[0, 1 - ROOT], inbox_sem.at[0])
        mine, partner = msg[...], inbox[0, 1 - ROOT]
        spot_b = lax.rem(spot, cross)
        between = (spot_b > 0) & (spot_b < cross - 1)
        masses = []
        for part in (mine, partner):
            found = jnp.where(between, part[1], 0.0)
            found = jnp.max(jnp.max(found, axis=1, keepdims=True), axis=0, keepdims=True)
            masses.append(jnp.broadcast_to(found, shape))
        spacings = [STEP / jnp.sqrt(v) for v in masses]
        walls = [wall_row / (jnp.sqrt(v) * law_scale) for v in masses]
        volumes = [
            (TIME_STEP / RAREFACTION) * NVEL * v * v * v * (0.5 / math.pi) for v in spacings
        ]

        own, other = mine, partner
        for part, (low, high) in enumerate([(1, middle + 1), (middle + 1, nz)]):
            settle(inbox.at[pl.ds(low, high - low)], inbox_sem.at[part + 1])
            for i in range(low, high):
                own += inbox[i, ROOT]
                other += inbox[i, 1 - ROOT]

        density = own[0] + other[0]
        per_density = 1.0 / density
        weight = masses[0] * own[0] + masses[1] * other[0]
        per_weight = 1.0 / weight
        flow_x = (own[2] + other[2]) * per_weight
        flow_y = (own[3] + other[3]) * per_weight
        flow_z = (own[4] + other[4]) * per_weight
        flow_square = flow_x * flow_x + flow_y * flow_y + flow_z * flow_z
        heat = 2.0 / 3.0 * (own[5] + other[5] - 0.5 * weight * flow_square) * per_density
        per_heat = 1.0 / heat
        for part, v, h, wall_v, volume, box in (
            (own, masses[0], spacings[0], walls[0], volumes[0], coef),
            (other, masses[1], spacings[1], walls[1], volumes[1], coef_other),
        ):
            sharp = v * per_heat
            top = part[0] * density * volume * sharp * jnp.sqrt(sharp * (0.5 / math.pi))
            slope = LOG2E * h * sharp
            curve = -0.5 * h * slope
            rows = [
                LOG2E * (jnp.log(top) - 0.5 * sharp * flow_square),
                slope * flow_x,
                slope * flow_y,
                slope * flow_z,
                curve,
                curve,
                1.0 - (TIME_STEP / RAREFACTION) * density,
                wall_v * (part[1] + sign * part[3]) + port_row,
            ]
            for i, values in enumerate(rows):
                box[:, i, :] = values

        coef_copy(0, 1 - ROOT, False, coef_send.at[0]).start()
        for copy in borders(range(1)) + served(first, coef_send.at[1]) + borders(first):
            copy.start()

    @pl.when(jnp.logical_not(is_root))
    def _():
        settle(coef, coef_recv)

    halo_cs = [
        halo_copy(coef.at[pairs - 1], halo_c, halo_c_send, halo_c_recv, 0),
        halo_copy(coef.at[0], halo_c, halo_c_send, halo_c_recv, 1),
    ]

    @pl.when(jnp.logical_not(is_first))
    def _():
        for copy in halo_cs:
            copy.start()

    def pass_on():
        return [coef_copy(z + k, s, True, pass_send.at[k - 1]) for k in range(1, FAN)]

    @pl.when(is_leader & (z > 0))
    def _():
        pl.semaphore_wait(ready, FAN - 1)
        for copy in pass_on():
            copy.start()

    tn = (((0,), (0,)), ((), ()))
    width = 256

    def collide(parts, rows, put, put_flux):
        side = lax.dot_general(parts, w[:, vel : vel + 256], tn, preferred_element_type=F32)
        stay = jnp.concatenate([side[:, :128]] * (width // 128), axis=1)
        if put_flux is not None:
            put_flux(side[:, 128:].reshape(2, cross, 128))
        for c in range(0, vel, width):
            power = lax.dot_general(parts, w[:, c : c + width], tn, preferred_element_type=F32)
            old = rows(c).reshape(2 * cross, width)
            put(c, (old * stay + jnp.exp2(power)).reshape(2, cross, width))

    for p in range(pairs):

        def rows(c, p=p):
            return d[2 * p : 2 * p + 2, :, c : c + width]

        def put(c, value, p=p):
            coll[2 * p + 1 : 2 * p + 3, :, c : c + width] = value

        def put_flux(value, p=p):
            flux[2 * p : 2 * p + 2] = value

        collide(pieces(coef[p]), rows, put, put_flux)

    @pl.when(is_root)
    def _():
        beyond = served(leaders, coef_send.at[2])
        for copy in served(others, coef_send.at[1]) + borders(others) + beyond:
            copy.start()

    level = lax.broadcasted_iota(jnp.int32, (cross, 128), 0)

    def stream(i):
        low_flux = flux[i, 0:1]
        high_flux = flux[i, cross - 1 : cross]
        for c in range(0, vel, 128):
            cols = slice(c, c + 128)
            here = coll[i + 1, :, cols]
            law = lane[5:6, cols]
            below = jnp.where(level == 0, low_flux * law, pltpu.roll(here, 1, 0))
            above = jnp.where(level == cross - 1, high_flux * law, pltpu.roll(here, cross - 1, 0))
            beside = jnp.where(lane[3:4, cols] > 0.0, coll[i, :, cols], coll[i + 2, :, cols])
            over = jnp.where(lane[4:5, cols] > 0.0, below, above)
            out[0, i, :, cols] = (
                lane[0:1, cols] * here + lane[1:2, cols] * beside + lane[2:3, cols] * over
            )

    for i in range(1, slab - 1):
        stream(i)

    settle(halo_d, halo_d_recv)
    settle(halo_c, halo_c_recv)
    spot = lax.broadcasted_iota(jnp.int32, (8, 128), 1)
    outer = jnp.where(spot < cross, halo_c[1], halo_c[0])

    def rows(c):
        return jnp.concatenate([halo_d[1:2, :, c : c + width], halo_d[0:1, :, c : c + width]], 0)

    def put(c, value):
        coll[slab + 1, :, c : c + width] = value[0]
        coll[0, :, c : c + width] = value[1]

    collide(pieces(outer), rows, put, None)
    stream(0)
    stream(slab - 1)

    settle(halo_d, halo_d_send)

    @pl.when(jnp.logical_not(is_first))
    def _():
        settle(halo_c, halo_c_send)

    @pl.when(jnp.logical_not(is_root))
    def _():
        settle(msg, msg_send)
        for copy in smalls[2:]:
            copy.wait()

    @pl.when(is_root)
    def _():
        settle(coef, coef_send.at[0])
        settle(d.at[0, pl.ds(0, 8 * (FAN - 1))], coef_send.at[1])
        settle(d.at[0, pl.ds(0, 8 * len(leaders))], coef_send.at[2])
        settle(d.at[0, pl.ds(0, 4 * FAN)], halo_r_send)

    @pl.when(is_leader & (z > 0))
    def _():
        for copy in pass_on():
            copy.wait_send()


def per_device(distribution, vel_order, species_mass, wall_mask, inflow_mask):
    _, slab, cross, vel = distribution.shape
    nz = lax.axis_size("vel")
    pairs = slab // 2
    hbm = pl.BlockSpec(memory_space=pltpu.HBM)

    def stay(array):
        return pltpu.with_memory_space_constraint(array, pltpu.HBM)

    dma = pltpu.SemaphoreType.DMA
    return pl.pallas_call(
        kernel,
        out_shape=jax.ShapeDtypeStruct(distribution.shape, F32),
        in_specs=[hbm] * 5,
        out_specs=pl.BlockSpec(memory_space=pltpu.VMEM),
        scratch_shapes=[
            pltpu.VMEM((slab, cross, vel), F32),
            pltpu.VMEM((1, vel), jnp.int32),
            pltpu.SMEM(species_mass.shape, jnp.int32),
            pltpu.SMEM((2, slab), jnp.int32),
            pltpu.SMEM((2, slab), jnp.int32),
            pltpu.VMEM((ROWS, pairs, 128), F32),
            pltpu.VMEM((nz, 2, ROWS, pairs, 128), F32),
            pltpu.VMEM((pairs, 8, 128), F32),
            pltpu.VMEM((pairs, 8, 128), F32),
            pltpu.VMEM((2, cross, vel), F32),
            pltpu.VMEM((2, 8, 128), F32),
            pltpu.VMEM((24, vel + 256), BF16),
            pltpu.VMEM((8, vel), F32),
            pltpu.VMEM((slab, cross, 128), F32),
            pltpu.VMEM((slab + 2, cross, vel), F32),
            dma(()),
            dma((4,)),
            dma(()),
            dma((3,)),
            dma((3,)),
            dma(()),
            dma((FAN - 1,)),
            dma(()),
            dma(()),
            dma(()),
            dma(()),
            dma(()),
            pltpu.SemaphoreType.REGULAR,
        ],
        compiler_params=pltpu.CompilerParams(
            collective_id=0, has_side_effects=True, vmem_limit_bytes=32 * 1024 * 1024
        ),
    )(
        stay(distribution),
        stay(vel_order.reshape(1, vel)),
        species_mass,
        stay(wall_mask.T),
        stay(inflow_mask.T),
    )


def solution(mesh):
    in_specs = (
        P("spec", ("groups", "space"), None, "vel"),
        P("vel"),
        P("spec"),
        P(("groups", "space"), None),
        P(("groups", "space"), None),
    )
    out_specs = P("spec", ("groups", "space"), None, "vel")
    return jax.shard_map(
        per_device, mesh=mesh, in_specs=in_specs, out_specs=out_specs, check_vma=False
    )
```

```python
import math

import jax
import jax.numpy as jnp
from jax import lax
from jax.experimental import pallas as pl
from jax.experimental.pallas import tpu as pltpu
from jax.sharding import PartitionSpec as P

NV = 32
NVEL = NV**3
BITS = NV.bit_length() - 1

TIME_STEP = 0.1
RAREFACTION = 0.5
PORT_DENSITY = 1.0
HALF_RANGE = 4.5
CENTRE = (NV - 1) / 2.0
STEP = 2.0 * HALF_RANGE / (NV - 1)
KAPPA = STEP * STEP
LOG2E = math.log2(math.e)

ROOT = 1
ROWS = 6
LOADS = 8
FAN = 4

F32 = jnp.float32
BF16 = jnp.bfloat16
MESH = pl.DeviceIdType.MESH


def pieces(rows):
    high = rows.astype(BF16).astype(F32)
    rest = rows - high
    middle = rest.astype(BF16).astype(F32)
    return jnp.concatenate([high, middle, rest - middle], axis=0).astype(BF16)


def lattice(order):
    index_a = lax.shift_right_logical(order, 2 * BITS).astype(F32)
    index_b = (lax.shift_right_logical(order, BITS) & (NV - 1)).astype(F32)
    index_e = (order & (NV - 1)).astype(F32)
    return index_a - CENTRE, index_b - CENTRE, index_e - CENTRE


def split_square(a, b, e):
    square = a * a + b * b + e * e
    coarse = jnp.floor(square * (1.0 / 32.0)) * 32.0
    return square, coarse, square - coarse


def rows_of(choices, shape):
    row = lax.broadcasted_iota(jnp.int32, shape, 0)
    out = choices[-1]
    for i in range(len(choices) - 2, -1, -1):
        out = jnp.where(row == i, choices[i], out)
    return out


def kernel(
    dist_in, order_in, mass_in, wall_in, inflow_in, coll, inner, lane, flux,
    d, order, mass, wall, inflow, msg, inbox, coef, coef_other, halo_d, halo_c,
    w,
    load_sem, small_sem, msg_send, inbox_sem, coef_send, coef_recv, pass_send,
    halo_d_send, halo_d_recv, halo_c_send, halo_c_recv, halo_r_send, ready,
):
    z, x, s = lax.axis_index("vel"), lax.axis_index("space"), lax.axis_index("spec")
    nz, nx = lax.axis_size("vel"), lax.axis_size("space")
    left, right = lax.rem(x + nx - 1, nx), lax.rem(x + 1, nx)
    slab, cross, vel = d.shape
    pairs = slab // 2
    is_root = (z == 0) & (s == ROOT)
    is_leader = lax.rem(z, FAN) == 0
    leader = z - lax.rem(z, FAN)
    middle = nz // 2 - 1
    rising = z <= nz // 2
    following = jnp.where(rising, z + FAN, z - FAN)
    preceding = jnp.where(rising, z - FAN, z + FAN)
    passes = is_leader & (z > 0)
    hands_on = passes & jnp.where(rising, following <= nz // 2, following > nz // 2)
    is_handed = passes & (z != FAN) & (z != nz - FAN)
    is_member = (z > FAN) & (leader != z)
    is_first = z < FAN

    barrier = pltpu.get_barrier_semaphore()

    def signal(sem, **where):
        pl.semaphore_signal(sem, inc=1, device_id=where, device_id_type=MESH)

    def settle(ref, sem):
        pltpu.make_async_copy(ref, ref, sem).wait()

    smalls = [
        pltpu.make_async_copy(order_in, order, small_sem.at[0]),
        pltpu.make_async_copy(mass_in, mass, small_sem.at[1]),
        pltpu.make_async_copy(wall_in, wall, small_sem.at[2]),
        pltpu.make_async_copy(inflow_in, inflow, small_sem.at[3]),
    ]
    loads = [
        pltpu.make_async_copy(
            dist_in.at[0, pl.ds(i, slab // LOADS)], d.at[pl.ds(i, slab // LOADS)], load_sem
        )
        for i in range(0, slab, slab // LOADS)
    ]
    for copy in smalls[:2] + loads + smalls[2:]:
        copy.start()

    signal(barrier, space=left)
    signal(barrier, space=right)

    @pl.when(is_root)
    def _():
        signal(barrier, spec=1 - s)

        def tell(i, carry):
            signal(barrier, vel=i, spec=0)
            signal(barrier, vel=i, spec=1)
            return carry

        lax.fori_loop(1, nz, tell, 0)

    @pl.when(is_first)
    def _():
        signal(barrier, space=left, vel=0, spec=ROOT)
        signal(barrier, space=right, vel=0, spec=ROOT)

    @pl.when(passes)
    def _():
        for k in range(1, FAN):
            signal(barrier, vel=z + k)

    @pl.when(hands_on)
    def _():
        signal(barrier, vel=following)

    smalls[0].wait()
    smalls[1].wait()
    a, b, e = lattice(jnp.broadcast_to(order[...], (8, vel)))
    square, coarse, fine = split_square(a, b, e)
    phi = rows_of([jnp.ones_like(a), jnp.abs(b), a, b, e, coarse, fine, fine], a.shape)
    phi = phi.astype(BF16)

    m = jnp.full((8, 128), mass[0], jnp.int32).astype(F32)
    root_m = jnp.sqrt(m)
    unit = jnp.full((8, 128), 1.0 / NVEL, F32)
    speed = root_m * (STEP / NVEL)
    energy = jnp.full((8, 128), 0.5 * KAPPA / NVEL, F32)
    scale = rows_of([unit, speed, speed, speed, speed, energy, energy, energy], m.shape)
    row = lax.broadcasted_iota(jnp.int32, (8, 128), 0)
    height = lax.broadcasted_iota(jnp.int32, (8, 128), 1) % cross
    amid = (height > 0) & (height < cross - 1)
    nt = (((1,), (1,)), ((), ()))
    settle(d, load_sem)
    for p in range(pairs):
        block = d[2 * p : 2 * p + 2].reshape(2 * cross, vel)
        high = block.astype(BF16)
        low = (block - high.astype(F32)).astype(BF16)
        part = lax.dot_general(phi, high, nt, preferred_element_type=F32)
        part += lax.dot_general(phi, low, nt, preferred_element_type=F32)
        part = (part + jnp.where(row == 5, pltpu.roll(part, 7, 0), 0.0)) * scale
        msg[:, p, :] = jnp.where((row == 1) & amid, m, part)[:ROWS]

    def one(flag):
        return jnp.where(flag, 1, 0)

    pl.semaphore_wait(
        barrier,
        2 + one(jnp.logical_not(is_root)) + one(is_member | is_handed) + 4 * FAN * one(is_root),
    )

    def to_root():
        return pltpu.make_async_remote_copy(
            src_ref=msg,
            dst_ref=inbox.at[z, s],
            send_sem=msg_send,
            recv_sem=inbox_sem.at[one(z > 0) + one(z > middle)],
            device_id={"vel": 0, "spec": ROOT},
            device_id_type=MESH,
        )

    @pl.when(jnp.logical_not(is_root))
    def _():
        to_root().start()

    def halo_copy(src, box, sends, recvs, side):
        return pltpu.make_async_remote_copy(
            src_ref=src,
            dst_ref=box.at[side],
            send_sem=sends,
            recv_sem=recvs,
            device_id={"space": right if side == 0 else left},
            device_id_type=MESH,
        )

    halo_ds = [
        halo_copy(d.at[slab - 1], halo_d, halo_d_send, halo_d_recv, 0),
        halo_copy(d.at[0], halo_d, halo_d_send, halo_d_recv, 1),
    ]
    for copy in halo_ds:
        copy.start()

    @pl.when(is_member | is_handed)
    def _():
        signal(ready, vel=jnp.where(is_handed, preceding, leader))

    speed_unit = (STEP / root_m)[:, :1]
    ones = jnp.ones((8, vel), F32)
    zeros = jnp.zeros((8, 128), F32)
    table = rows_of([ones, a, b, e, coarse, fine, 0.0 * ones, 0.0 * ones], ones.shape)
    keep = jnp.where(row == 6, 1.0, zeros)
    emit = jnp.where(row == 7, 1.0, zeros)
    table = jnp.concatenate([table, keep, emit], axis=1)
    w[...] = jnp.concatenate([table, table, table], axis=0).astype(BF16)
    go_x = TIME_STEP * speed_unit * jnp.abs(a)
    go_y = TIME_STEP * speed_unit * jnp.abs(b)
    law_unit = NVEL * (KAPPA / (2.0 * math.pi)) ** 1.5
    law = law_unit * jnp.exp(-0.5 * KAPPA * square)
    lane[...] = rows_of([1.0 - go_x - go_y, go_x, go_y, a, b, law, law, law], ones.shape)

    def coef_copy(i, core, own, sem):
        return pltpu.make_async_remote_copy(
            src_ref=coef if own else coef_other,
            dst_ref=coef,
            send_sem=sem,
            recv_sem=coef_recv,
            device_id={"vel": i, "spec": core},
            device_id_type=MESH,
        )

    def served(places, sem):
        nearest = sorted(places, key=lambda i: min(i, nz - i))
        return [coef_copy(i, core, core == ROOT, sem) for i in nearest for core in (ROOT, 1 - ROOT)]

    first, others, leaders = range(1, 2), range(2, FAN), sorted({FAN, nz - FAN})

    def borders(places):
        return [
            pltpu.make_async_remote_copy(
                src_ref=(coef if core == ROOT else coef_other).at[pairs - 1 if side == 0 else 0],
                dst_ref=halo_c.at[side],
                send_sem=halo_r_send,
                recv_sem=halo_c_recv,
                device_id={"space": right if side == 0 else left, "vel": i, "spec": core},
                device_id_type=MESH,
            )
            for i in places
            for core in (ROOT, 1 - ROOT)
            for side in range(2)
        ]


    @pl.when(is_root)
    def _():
        for copy in smalls[2:]:
            copy.wait()
        shape = (pairs, 128)
        spot = lax.broadcasted_iota(jnp.int32, shape, 0) * 128
        spot = spot + lax.broadcasted_iota(jnp.int32, shape, 1)
        wall_row = jnp.zeros(shape, F32)
        port_row = jnp.zeros(shape, F32)
        for i in range(slab):
            for side in range(2):
                here = spot == i * cross + side * (cross - 1)
                wall_row = jnp.where(here, jnp.full(shape, wall[side, i], jnp.int32).astype(F32), wall_row)
                port_row = jnp.where(here, jnp.full(shape, inflow[side, i], jnp.int32).astype(F32), port_row)
        port_row = port_row * PORT_DENSITY
        offset = spot.astype(F32) - CENTRE
        bell = jnp.where(spot < NV, jnp.exp(-0.5 * KAPPA * offset * offset), 0.0)
        bell_sum = jnp.sum(jnp.sum(bell, axis=1, keepdims=True), axis=0, keepdims=True)
        flow = jnp.maximum(offset, 0.0) * bell
        flow_sum = jnp.sum(jnp.sum(flow, axis=1, keepdims=True), axis=0, keepdims=True)
        sign = jnp.where(lax.rem(spot, cross) == 0, -1.0, 1.0)
        law_scale = (2.0 * STEP) * (KAPPA / (2.0 * math.pi)) ** 1.5 * flow_sum * bell_sum * bell_sum

        settle(inbox.at[0, 1 - ROOT], inbox_sem.at[0])
        mine, partner = msg[...], inbox[0, 1 - ROOT]
        spot_b = lax.rem(spot, cross)
        between = (spot_b > 0) & (spot_b < cross - 1)
        masses = []
        for part in (mine, partner):
            found = jnp.where(between, part[1], 0.0)
            found = jnp.max(jnp.max(found, axis=1, keepdims=True), axis=0, keepdims=True)
            masses.append(jnp.broadcast_to(found, shape))
        spacings = [STEP / jnp.sqrt(v) for v in masses]
        walls = [wall_row / (jnp.sqrt(v) * law_scale) for v in masses]
        volumes = [
            (TIME_STEP / RAREFACTION) * NVEL * v * v * v * (0.5 / math.pi) for v in spacings
        ]

        own, other = mine, partner
        for part, (low, high) in enumerate([(1, middle + 1), (middle + 1, nz)]):
            settle(inbox.at[pl.ds(low, high - low)], inbox_sem.at[part + 1])
            for i in range(low, high):
                own += inbox[i, ROOT]
                other += inbox[i, 1 - ROOT]

        density = own[0] + other[0]
        per_density = 1.0 / density
        weight = masses[0] * own[0] + masses[1] * other[0]
        per_weight = 1.0 / weight
        flow_x = (own[2] + other[2]) * per_weight
        flow_y = (own[3] + other[3]) * per_weight
        flow_z = (own[4] + other[4]) * per_weight
        flow_square = flow_x * flow_x + flow_y * flow_y + flow_z * flow_z
        heat = 2.0 / 3.0 * (own[5] + other[5] - 0.5 * weight * flow_square) * per_density
        per_heat = 1.0 / heat
        for part, v, h, wall_v, volume, box in (
            (own, masses[0], spacings[0], walls[0], volumes[0], coef),
            (other, masses[1], spacings[1], walls[1], volumes[1], coef_other),
        ):
            sharp = v * per_heat
            top = part[0] * density * volume * sharp * jnp.sqrt(sharp * (0.5 / math.pi))
            slope = LOG2E * h * sharp
            curve = -0.5 * h * slope
            rows = [
                LOG2E * (jnp.log(top) - 0.5 * sharp * flow_square),
                slope * flow_x,
                slope * flow_y,
                slope * flow_z,
                curve,
                curve,
                1.0 - (TIME_STEP / RAREFACTION) * density,
                wall_v * (part[1] + sign * part[3]) + port_row,
            ]
            for i, values in enumerate(rows):
                box[:, i, :] = values

        coef_copy(0, 1 - ROOT, False, coef_send.at[0]).start()
        for copy in borders(range(1)) + served(first, coef_send.at[1]) + borders(first):
            copy.start()

    @pl.when(jnp.logical_not(is_root))
    def _():
        settle(coef, coef_recv)

    halo_cs = [
        halo_copy(coef.at[pairs - 1], halo_c, halo_c_send, halo_c_recv, 0),
        halo_copy(coef.at[0], halo_c, halo_c_send, halo_c_recv, 1),
    ]

    @pl.when(jnp.logical_not(is_first))
    def _():
        for copy in halo_cs:
            copy.start()

    def pass_on():
        return [coef_copy(z + k, s, True, pass_send.at[k - 1]) for k in range(1, FAN)]

    def hand_on():
        return coef_copy(following, s, True, pass_send.at[FAN - 1])

    @pl.when(passes)
    def _():
        pl.semaphore_wait(ready, FAN - 1 + one(hands_on))
        for copy in pass_on():
            copy.start()

    @pl.when(hands_on)
    def _():
        hand_on().start()

    tn = (((0,), (0,)), ((), ()))
    width = 256

    def collide(parts, rows, put, put_flux):
        side = lax.dot_general(parts, w[:, vel : vel + 256], tn, preferred_element_type=F32)
        stay = jnp.concatenate([side[:, :128]] * (width // 128), axis=1)
        if put_flux is not None:
            put_flux(side[:, 128:].reshape(2, cross, 128))
        for c in range(0, vel, width):
            power = lax.dot_general(parts, w[:, c : c + width], tn, preferred_element_type=F32)
            old = rows(c).reshape(2 * cross, width)
            put(c, (old * stay + jnp.exp2(power)).reshape(2, cross, width))

    for p in range(pairs):

        def rows(c, p=p):
            return d[2 * p : 2 * p + 2, :, c : c + width]

        def put(c, value, p=p):
            coll[2 * p + 1 : 2 * p + 3, :, c : c + width] = value

        def put_flux(value, p=p):
            flux[2 * p : 2 * p + 2] = value

        collide(pieces(coef[p]), rows, put, put_flux)

    @pl.when(is_root)
    def _():
        beyond = served(leaders, coef_send.at[2])
        for copy in served(others, coef_send.at[1]) + borders(others) + beyond:
            copy.start()

    for i in range(1, slab - 1):
        stream(coll, lane, flux, i, inner.at[i - 1])

    settle(halo_d, halo_d_recv)
    settle(halo_c, halo_c_recv)
    spot = lax.broadcasted_iota(jnp.int32, (8, 128), 1)
    outer = jnp.where(spot < cross, halo_c[1], halo_c[0])

    def rows(c):
        return jnp.concatenate([halo_d[1:2, :, c : c + width], halo_d[0:1, :, c : c + width]], 0)

    def put(c, value):
        coll[slab + 1, :, c : c + width] = value[0]
        coll[0, :, c : c + width] = value[1]

    collide(pieces(outer), rows, put, None)

    settle(halo_d, halo_d_send)

    @pl.when(jnp.logical_not(is_first))
    def _():
        settle(halo_c, halo_c_send)

    @pl.when(jnp.logical_not(is_root))
    def _():
        settle(msg, msg_send)
        for copy in smalls[2:]:
            copy.wait()

    @pl.when(is_root)
    def _():
        settle(coef, coef_send.at[0])
        settle(d.at[0, pl.ds(0, 8 * (FAN - 1))], coef_send.at[1])
        settle(d.at[0, pl.ds(0, 8 * len(leaders))], coef_send.at[2])
        settle(d.at[0, pl.ds(0, 4 * FAN)], halo_r_send)

    @pl.when(passes)
    def _():
        for copy in pass_on():
            copy.wait_send()

    @pl.when(hands_on)
    def _():
        hand_on().wait_send()


def stream(coll, lane, flux, i, out):
    _, cross, vel = coll.shape
    level = lax.broadcasted_iota(jnp.int32, (cross, 128), 0)
    low_flux = flux[i, 0:1]
    high_flux = flux[i, cross - 1 : cross]
    for c in range(0, vel, 128):
        cols = slice(c, c + 128)
        here = coll[i + 1, :, cols]
        law = lane[5:6, cols]
        below = jnp.where(level == 0, low_flux * law, pltpu.roll(here, 1, 0))
        above = jnp.where(level == cross - 1, high_flux * law, pltpu.roll(here, cross - 1, 0))
        beside = jnp.where(lane[3:4, cols] > 0.0, coll[i, :, cols], coll[i + 2, :, cols])
        over = jnp.where(lane[4:5, cols] > 0.0, below, above)
        out[:, cols] = lane[0:1, cols] * here + lane[1:2, cols] * beside + lane[2:3, cols] * over


def finish(coll, inner, lane, flux, out, edge, sem):
    slab = flux.shape[0]
    copies = [pltpu.make_async_copy(inner, out.at[0, pl.ds(1, slab - 2)], sem.at[2])]
    copies[0].start()
    for k, i in enumerate((0, slab - 1)):
        stream(coll, lane, flux, i, edge.at[k])
        copies.append(pltpu.make_async_copy(edge.at[k], out.at[0, i], sem.at[k]))
        copies[-1].start()
    for copy in copies:
        copy.wait()


def per_device(distribution, vel_order, species_mass, wall_mask, inflow_mask):
    _, slab, cross, vel = distribution.shape
    nz = lax.axis_size("vel")
    pairs = slab // 2
    hbm = pl.BlockSpec(memory_space=pltpu.HBM)

    def stay(array):
        return pltpu.with_memory_space_constraint(array, pltpu.HBM)

    dma = pltpu.SemaphoreType.DMA
    vmem = pl.BlockSpec(memory_space=pltpu.VMEM)
    passed = [
        jax.ShapeDtypeStruct(shape, F32)
        for shape in [
            (slab + 2, cross, vel),
            (slab - 2, cross, vel),
            (8, vel),
            (slab, cross, 128),
        ]
    ]
    parts = pl.pallas_call(
        kernel,
        out_shape=passed,
        in_specs=[hbm] * 5,
        out_specs=[vmem] * 4,
        scratch_shapes=[
            pltpu.VMEM((slab, cross, vel), F32),
            pltpu.VMEM((1, vel), jnp.int32),
            pltpu.SMEM(species_mass.shape, jnp.int32),
            pltpu.SMEM((2, slab), jnp.int32),
            pltpu.SMEM((2, slab), jnp.int32),
            pltpu.VMEM((ROWS, pairs, 128), F32),
            pltpu.VMEM((nz, 2, ROWS, pairs, 128), F32),
            pltpu.VMEM((pairs, 8, 128), F32),
            pltpu.VMEM((pairs, 8, 128), F32),
            pltpu.VMEM((2, cross, vel), F32),
            pltpu.VMEM((2, 8, 128), F32),
            pltpu.VMEM((24, vel + 256), BF16),
            dma(()),
            dma((4,)),
            dma(()),
            dma((3,)),
            dma((3,)),
            dma(()),
            dma((FAN,)),
            dma(()),
            dma(()),
            dma(()),
            dma(()),
            dma(()),
            pltpu.SemaphoreType.REGULAR,
        ],
        compiler_params=pltpu.CompilerParams(
            collective_id=0, has_side_effects=True, vmem_limit_bytes=32 * 1024 * 1024
        ),
    )(
        stay(distribution),
        stay(vel_order.reshape(1, vel)),
        species_mass,
        stay(wall_mask.T),
        stay(inflow_mask.T),
    )
    return pl.pallas_call(
        finish,
        out_shape=jax.ShapeDtypeStruct(distribution.shape, F32),
        in_specs=[vmem] * 4,
        out_specs=hbm,
        scratch_shapes=[pltpu.VMEM((2, cross, vel), F32), dma((3,))],
        compiler_params=pltpu.CompilerParams(vmem_limit_bytes=16 * 1024 * 1024),
    )(*parts)


def solution(mesh):
    in_specs = (
        P("spec", ("groups", "space"), None, "vel"),
        P("vel"),
        P("spec"),
        P(("groups", "space"), None),
        P(("groups", "space"), None),
    )
    out_specs = P("spec", ("groups", "space"), None, "vel")
    return jax.shard_map(
        per_device, mesh=mesh, in_specs=in_specs, out_specs=out_specs, check_vma=False
    )
```

```python
import math

import jax
import jax.numpy as jnp
from jax import lax
from jax.experimental import pallas as pl
from jax.experimental.pallas import tpu as pltpu
from jax.sharding import PartitionSpec as P

NV = 32
NVEL = NV**3
BITS = NV.bit_length() - 1

TIME_STEP = 0.1
RAREFACTION = 0.5
PORT_DENSITY = 1.0
HALF_RANGE = 4.5
CENTRE = (NV - 1) / 2.0
STEP = 2.0 * HALF_RANGE / (NV - 1)
KAPPA = STEP * STEP
LOG2E = math.log2(math.e)

ROOT = 1
ROWS = 6
SINGLE = 4
LOADS = 8
FAN = 4

F32 = jnp.float32
BF16 = jnp.bfloat16
MESH = pl.DeviceIdType.MESH


def pieces(rows):
    high = rows.astype(BF16).astype(F32)
    rest = rows - high
    middle = rest.astype(BF16).astype(F32)
    return jnp.concatenate([high, middle, rest - middle], axis=0).astype(BF16)


def lattice(order):
    index_a = lax.shift_right_logical(order, 2 * BITS).astype(F32)
    index_b = (lax.shift_right_logical(order, BITS) & (NV - 1)).astype(F32)
    index_e = (order & (NV - 1)).astype(F32)
    return index_a - CENTRE, index_b - CENTRE, index_e - CENTRE


def split_square(a, b, e):
    square = a * a + b * b + e * e
    coarse = jnp.floor(square * (1.0 / 32.0)) * 32.0
    return square, coarse, square - coarse


def rows_of(choices, shape):
    row = lax.broadcasted_iota(jnp.int32, shape, 0)
    out = choices[-1]
    for i in range(len(choices) - 2, -1, -1):
        out = jnp.where(row == i, choices[i], out)
    return out


def kernel(
    dist_in, order_in, mass_in, wall_in, inflow_in, coll, inner, lane, flux,
    d, order, mass, wall, inflow, msg, inbox, relay, coef, coef_other, halo_d, halo_c,
    w,
    load_sem, small_sem, msg_send, inbox_sem, relay_sem, coef_send, coef_recv, pass_send,
    halo_d_send, halo_d_recv, halo_c_send, halo_c_recv, halo_r_send, ready,
):
    z, x, s = lax.axis_index("vel"), lax.axis_index("space"), lax.axis_index("spec")
    nz, nx = lax.axis_size("vel"), lax.axis_size("space")
    left, right = lax.rem(x + nx - 1, nx), lax.rem(x + 1, nx)
    slab, cross, vel = d.shape
    pairs = slab // 2
    is_root = (z == 0) & (s == ROOT)
    is_leader = lax.rem(z, FAN) == 0
    leader = z - lax.rem(z, FAN)
    middle = nz // 2 - 1
    couples = (nz - SINGLE - middle - 1) // 2
    singles = middle + 1 + 2 * couples
    is_paired = (z > middle) & (z < singles)
    is_giver = is_paired & (lax.rem(z - middle, 2) == 1)
    is_taker = is_paired & (lax.rem(z - middle, 2) == 0)
    senders = middle + 1 + couples + nz - singles
    slot = jnp.where(is_paired, middle + 1 + (z - middle - 1) // 2, jnp.where(z > middle, z - couples, z))
    rising = z <= nz // 2
    following = jnp.where(rising, z + FAN, z - FAN)
    preceding = jnp.where(rising, z - FAN, z + FAN)
    passes = is_leader & (z > 0)
    hands_on = passes & jnp.where(rising, following <= nz // 2, following > nz // 2)
    is_handed = passes & (z != FAN) & (z != nz - FAN)
    is_member = (z > FAN) & (leader != z)
    is_first = z < FAN

    barrier = pltpu.get_barrier_semaphore()

    def signal(sem, **where):
        pl.semaphore_signal(sem, inc=1, device_id=where, device_id_type=MESH)

    def settle(ref, sem):
        pltpu.make_async_copy(ref, ref, sem).wait()

    smalls = [
        pltpu.make_async_copy(order_in, order, small_sem.at[0]),
        pltpu.make_async_copy(mass_in, mass, small_sem.at[1]),
        pltpu.make_async_copy(wall_in, wall, small_sem.at[2]),
        pltpu.make_async_copy(inflow_in, inflow, small_sem.at[3]),
    ]
    loads = [
        pltpu.make_async_copy(
            dist_in.at[0, pl.ds(i, slab // LOADS)], d.at[pl.ds(i, slab // LOADS)], load_sem
        )
        for i in range(0, slab, slab // LOADS)
    ]
    for copy in smalls[:2] + loads + smalls[2:]:
        copy.start()

    signal(barrier, space=left)
    signal(barrier, space=right)

    @pl.when(is_root)
    def _():
        signal(barrier, spec=1 - s)

        def tell(i, carry):
            @pl.when((i <= middle) | (i >= singles) | (lax.rem(i - middle, 2) == 0))
            def _():
                signal(barrier, vel=i, spec=0)
                signal(barrier, vel=i, spec=1)

            return carry

        lax.fori_loop(1, nz, tell, 0)

    @pl.when(is_taker)
    def _():
        signal(barrier, vel=z - 1)

    @pl.when(is_first)
    def _():
        signal(barrier, space=left, vel=0, spec=ROOT)
        signal(barrier, space=right, vel=0, spec=ROOT)

    @pl.when(passes)
    def _():
        for k in range(1, FAN):
            signal(barrier, vel=z + k)

    @pl.when(hands_on)
    def _():
        signal(barrier, vel=following)

    smalls[0].wait()
    smalls[1].wait()
    a, b, e = lattice(jnp.broadcast_to(order[...], (8, vel)))
    square, coarse, fine = split_square(a, b, e)
    phi = rows_of([jnp.ones_like(a), jnp.abs(b), a, b, e, coarse, fine, fine], a.shape)
    phi = phi.astype(BF16)

    m = jnp.full((8, 128), mass[0], jnp.int32).astype(F32)
    root_m = jnp.sqrt(m)
    unit = jnp.full((8, 128), 1.0 / NVEL, F32)
    speed = root_m * (STEP / NVEL)
    energy = jnp.full((8, 128), 0.5 * KAPPA / NVEL, F32)
    scale = rows_of([unit, speed, speed, speed, speed, energy, energy, energy], m.shape)
    row = lax.broadcasted_iota(jnp.int32, (8, 128), 0)
    height = lax.broadcasted_iota(jnp.int32, (8, 128), 1) % cross
    amid = (height > 0) & (height < cross - 1)
    nt = (((1,), (1,)), ((), ()))
    settle(d, load_sem)
    for p in range(pairs):
        block = d[2 * p : 2 * p + 2].reshape(2 * cross, vel)
        high = block.astype(BF16)
        low = (block - high.astype(F32)).astype(BF16)
        part = lax.dot_general(phi, high, nt, preferred_element_type=F32)
        part += lax.dot_general(phi, low, nt, preferred_element_type=F32)
        part = (part + jnp.where(row == 5, pltpu.roll(part, 7, 0), 0.0)) * scale
        msg[:, p, :] = jnp.where((row == 1) & amid, m, part)[:ROWS]

    def one(flag):
        return jnp.where(flag, 1, 0)

    pl.semaphore_wait(
        barrier,
        2 + one(jnp.logical_not(is_root)) + one(is_member | is_handed) + 4 * FAN * one(is_root),
    )

    def to_root():
        return pltpu.make_async_remote_copy(
            src_ref=msg,
            dst_ref=inbox.at[slot, s],
            send_sem=msg_send,
            recv_sem=inbox_sem.at[one(z > 0) + one(z > middle)],
            device_id={"vel": 0, "spec": ROOT},
            device_id_type=MESH,
        )

    def to_taker():
        return pltpu.make_async_remote_copy(
            src_ref=msg,
            dst_ref=relay,
            send_sem=msg_send,
            recv_sem=relay_sem,
            device_id={"vel": z + 1},
            device_id_type=MESH,
        )

    @pl.when(jnp.logical_not(is_root | is_paired))
    def _():
        to_root().start()

    @pl.when(is_giver)
    def _():
        to_taker().start()

    def halo_copy(src, box, sends, recvs, side):
        return pltpu.make_async_remote_copy(
            src_ref=src,
            dst_ref=box.at[side],
            send_sem=sends,
            recv_sem=recvs,
            device_id={"space": right if side == 0 else left},
            device_id_type=MESH,
        )

    halo_ds = [
        halo_copy(d.at[slab - 1], halo_d, halo_d_send, halo_d_recv, 0),
        halo_copy(d.at[0], halo_d, halo_d_send, halo_d_recv, 1),
    ]
    for copy in halo_ds:
        copy.start()

    @pl.when(is_member | is_handed)
    def _():
        signal(ready, vel=jnp.where(is_handed, preceding, leader))

    @pl.when(is_taker)
    def _():
        settle(relay, relay_sem)
        msg[...] += relay[...]
        to_root().start()

    speed_unit = (STEP / root_m)[:, :1]
    ones = jnp.ones((8, vel), F32)
    zeros = jnp.zeros((8, 128), F32)
    table = rows_of([ones, a, b, e, coarse, fine, 0.0 * ones, 0.0 * ones], ones.shape)
    keep = jnp.where(row == 6, 1.0, zeros)
    emit = jnp.where(row == 7, 1.0, zeros)
    table = jnp.concatenate([table, keep, emit], axis=1)
    w[...] = jnp.concatenate([table, table, table], axis=0).astype(BF16)
    go_x = TIME_STEP * speed_unit * jnp.abs(a)
    go_y = TIME_STEP * speed_unit * jnp.abs(b)
    law_unit = NVEL * (KAPPA / (2.0 * math.pi)) ** 1.5
    law = law_unit * jnp.exp(-0.5 * KAPPA * square)
    lane[...] = rows_of([1.0 - go_x - go_y, go_x, go_y, a, b, law, law, law], ones.shape)

    def coef_copy(i, core, own, sem):
        return pltpu.make_async_remote_copy(
            src_ref=coef if own else coef_other,
            dst_ref=coef,
            send_sem=sem,
            recv_sem=coef_recv,
            device_id={"vel": i, "spec": core},
            device_id_type=MESH,
        )

    def served(places, sem):
        nearest = sorted(places, key=lambda i: min(i, nz - i))
        return [coef_copy(i, core, core == ROOT, sem) for i in nearest for core in (ROOT, 1 - ROOT)]

    first, others, leaders = range(1, 2), range(2, FAN), sorted({FAN, nz - FAN})

    def borders(places):
        return [
            pltpu.make_async_remote_copy(
                src_ref=(coef if core == ROOT else coef_other).at[pairs - 1 if side == 0 else 0],
                dst_ref=halo_c.at[side],
                send_sem=halo_r_send,
                recv_sem=halo_c_recv,
                device_id={"space": right if side == 0 else left, "vel": i, "spec": core},
                device_id_type=MESH,
            )
            for i in places
            for core in (ROOT, 1 - ROOT)
            for side in range(2)
        ]


    @pl.when(is_root)
    def _():
        for copy in smalls[2:]:
            copy.wait()
        shape = (pairs, 128)
        spot = lax.broadcasted_iota(jnp.int32, shape, 0) * 128
        spot = spot + lax.broadcasted_iota(jnp.int32, shape, 1)
        wall_row = jnp.zeros(shape, F32)
        port_row = jnp.zeros(shape, F32)
        for i in range(slab):
            for side in range(2):
                here = spot == i * cross + side * (cross - 1)
                wall_row = jnp.where(here, jnp.full(shape, wall[side, i], jnp.int32).astype(F32), wall_row)
                port_row = jnp.where(here, jnp.full(shape, inflow[side, i], jnp.int32).astype(F32), port_row)
        port_row = port_row * PORT_DENSITY
        offset = spot.astype(F32) - CENTRE
        bell = jnp.where(spot < NV, jnp.exp(-0.5 * KAPPA * offset * offset), 0.0)
        bell_sum = jnp.sum(jnp.sum(bell, axis=1, keepdims=True), axis=0, keepdims=True)
        flow = jnp.maximum(offset, 0.0) * bell
        flow_sum = jnp.sum(jnp.sum(flow, axis=1, keepdims=True), axis=0, keepdims=True)
        sign = jnp.where(lax.rem(spot, cross) == 0, -1.0, 1.0)
        law_scale = (2.0 * STEP) * (KAPPA / (2.0 * math.pi)) ** 1.5 * flow_sum * bell_sum * bell_sum

        settle(inbox.at[0, 1 - ROOT], inbox_sem.at[0])
        mine, partner = msg[...], inbox[0, 1 - ROOT]
        spot_b = lax.rem(spot, cross)
        between = (spot_b > 0) & (spot_b < cross - 1)
        masses = []
        for part in (mine, partner):
            found = jnp.where(between, part[1], 0.0)
            found = jnp.max(jnp.max(found, axis=1, keepdims=True), axis=0, keepdims=True)
            masses.append(jnp.broadcast_to(found, shape))
        spacings = [STEP / jnp.sqrt(v) for v in masses]
        walls = [wall_row / (jnp.sqrt(v) * law_scale) for v in masses]
        volumes = [
            (TIME_STEP / RAREFACTION) * NVEL * v * v * v * (0.5 / math.pi) for v in spacings
        ]

        own, other = mine, partner
        for part, (low, high) in enumerate([(1, middle + 1), (middle + 1, senders)]):
            settle(inbox.at[pl.ds(low, high - low)], inbox_sem.at[part + 1])
            for i in range(low, high):
                own += inbox[i, ROOT]
                other += inbox[i, 1 - ROOT]

        density = own[0] + other[0]
        per_density = 1.0 / density
        weight = masses[0] * own[0] + masses[1] * other[0]
        per_weight = 1.0 / weight
        flow_x = (own[2] + other[2]) * per_weight
        flow_y = (own[3] + other[3]) * per_weight
        flow_z = (own[4] + other[4]) * per_weight
        flow_square = flow_x * flow_x + flow_y * flow_y + flow_z * flow_z
        heat = 2.0 / 3.0 * (own[5] + other[5] - 0.5 * weight * flow_square) * per_density
        per_heat = 1.0 / heat
        for part, v, h, wall_v, volume, box in (
            (own, masses[0], spacings[0], walls[0], volumes[0], coef),
            (other, masses[1], spacings[1], walls[1], volumes[1], coef_other),
        ):
            sharp = v * per_heat
            top = part[0] * density * volume * sharp * jnp.sqrt(sharp * (0.5 / math.pi))
            slope = LOG2E * h * sharp
            curve = -0.5 * h * slope
            rows = [
                LOG2E * (jnp.log(top) - 0.5 * sharp * flow_square),
                slope * flow_x,
                slope * flow_y,
                slope * flow_z,
                curve,
                curve,
                1.0 - (TIME_STEP / RAREFACTION) * density,
                wall_v * (part[1] + sign * part[3]) + port_row,
            ]
            for i, values in enumerate(rows):
                box[:, i, :] = values

        coef_copy(0, 1 - ROOT, False, coef_send.at[0]).start()
        for copy in borders(range(1)) + served(first, coef_send.at[1]) + borders(first):
            copy.start()

    @pl.when(jnp.logical_not(is_root))
    def _():
        settle(coef, coef_recv)

    halo_cs = [
        halo_copy(coef.at[pairs - 1], halo_c, halo_c_send, halo_c_recv, 0),
        halo_copy(coef.at[0], halo_c, halo_c_send, halo_c_recv, 1),
    ]

    @pl.when(jnp.logical_not(is_first))
    def _():
        for copy in halo_cs:
            copy.start()

    def pass_on():
        return [coef_copy(z + k, s, True, pass_send.at[k - 1]) for k in range(1, FAN)]

    def hand_on():
        return coef_copy(following, s, True, pass_send.at[FAN - 1])

    @pl.when(passes)
    def _():
        pl.semaphore_wait(ready, FAN - 1 + one(hands_on))
        for copy in pass_on():
            copy.start()

    @pl.when(hands_on)
    def _():
        hand_on().start()

    tn = (((0,), (0,)), ((), ()))
    width = 256

    def collide(parts, rows, put, put_flux):
        side = lax.dot_general(parts, w[:, vel : vel + 256], tn, preferred_element_type=F32)
        stay = jnp.concatenate([side[:, :128]] * (width // 128), axis=1)
        if put_flux is not None:
            put_flux(side[:, 128:].reshape(2, cross, 128))
        for c in range(0, vel, width):
            power = lax.dot_general(parts, w[:, c : c + width], tn, preferred_element_type=F32)
            old = rows(c).reshape(2 * cross, width)
            put(c, (old * stay + jnp.exp2(power)).reshape(2, cross, width))

    for p in range(pairs):

        def rows(c, p=p):
            return d[2 * p : 2 * p + 2, :, c : c + width]

        def put(c, value, p=p):
            coll[2 * p + 1 : 2 * p + 3, :, c : c + width] = value

        def put_flux(value, p=p):
            flux[2 * p : 2 * p + 2] = value

        collide(pieces(coef[p]), rows, put, put_flux)

    @pl.when(is_root)
    def _():
        beyond = served(leaders, coef_send.at[2])
        for copy in served(others, coef_send.at[1]) + borders(others) + beyond:
            copy.start()

    for i in range(1, slab - 1):
        stream(coll, lane, flux, i, inner.at[i - 1])

    settle(halo_d, halo_d_recv)
    settle(halo_c, halo_c_recv)
    spot = lax.broadcasted_iota(jnp.int32, (8, 128), 1)
    outer = jnp.where(spot < cross, halo_c[1], halo_c[0])

    def rows(c):
        return jnp.concatenate([halo_d[1:2, :, c : c + width], halo_d[0:1, :, c : c + width]], 0)

    def put(c, value):
        coll[slab + 1, :, c : c + width] = value[0]
        coll[0, :, c : c + width] = value[1]

    collide(pieces(outer), rows, put, None)

    settle(halo_d, halo_d_send)

    @pl.when(jnp.logical_not(is_first))
    def _():
        settle(halo_c, halo_c_send)

    @pl.when(jnp.logical_not(is_root))
    def _():
        settle(msg, msg_send)
        for copy in smalls[2:]:
            copy.wait()

    @pl.when(is_root)
    def _():
        settle(coef, coef_send.at[0])
        settle(d.at[0, pl.ds(0, 8 * (FAN - 1))], coef_send.at[1])
        settle(d.at[0, pl.ds(0, 8 * len(leaders))], coef_send.at[2])
        settle(d.at[0, pl.ds(0, 4 * FAN)], halo_r_send)

    @pl.when(passes)
    def _():
        for copy in pass_on():
            copy.wait_send()

    @pl.when(hands_on)
    def _():
        hand_on().wait_send()


def stream(coll, lane, flux, i, out):
    _, cross, vel = coll.shape
    level = lax.broadcasted_iota(jnp.int32, (cross, 128), 0)
    low_flux = flux[i, 0:1]
    high_flux = flux[i, cross - 1 : cross]
    for c in range(0, vel, 128):
        cols = slice(c, c + 128)
        here = coll[i + 1, :, cols]
        law = lane[5:6, cols]
        below = jnp.where(level == 0, low_flux * law, pltpu.roll(here, 1, 0))
        above = jnp.where(level == cross - 1, high_flux * law, pltpu.roll(here, cross - 1, 0))
        beside = jnp.where(lane[3:4, cols] > 0.0, coll[i, :, cols], coll[i + 2, :, cols])
        over = jnp.where(lane[4:5, cols] > 0.0, below, above)
        out[:, cols] = lane[0:1, cols] * here + lane[1:2, cols] * beside + lane[2:3, cols] * over


def finish(coll, inner, lane, flux, out, edge, sem):
    slab = flux.shape[0]
    for i in range(slab - 2):
        pltpu.make_async_copy(inner.at[i], out.at[0, i + 1], sem.at[2]).start()
    copies = [pltpu.make_async_copy(inner, out.at[0, pl.ds(1, slab - 2)], sem.at[2])]
    for k, i in enumerate((0, slab - 1)):
        stream(coll, lane, flux, i, edge.at[k])
        copies.append(pltpu.make_async_copy(edge.at[k], out.at[0, i], sem.at[k]))
        copies[-1].start()
    for copy in copies:
        copy.wait()


def per_device(distribution, vel_order, species_mass, wall_mask, inflow_mask):
    _, slab, cross, vel = distribution.shape
    nz = lax.axis_size("vel")
    pairs = slab // 2
    hbm = pl.BlockSpec(memory_space=pltpu.HBM)

    def stay(array):
        return pltpu.with_memory_space_constraint(array, pltpu.HBM)

    dma = pltpu.SemaphoreType.DMA
    vmem = pl.BlockSpec(memory_space=pltpu.VMEM)
    passed = [
        jax.ShapeDtypeStruct(shape, F32)
        for shape in [
            (slab + 2, cross, vel),
            (slab - 2, cross, vel),
            (8, vel),
            (slab, cross, 128),
        ]
    ]
    parts = pl.pallas_call(
        kernel,
        out_shape=passed,
        in_specs=[hbm] * 5,
        out_specs=[vmem] * 4,
        scratch_shapes=[
            pltpu.VMEM((slab, cross, vel), F32),
            pltpu.VMEM((1, vel), jnp.int32),
            pltpu.SMEM(species_mass.shape, jnp.int32),
            pltpu.SMEM((2, slab), jnp.int32),
            pltpu.SMEM((2, slab), jnp.int32),
            pltpu.VMEM((ROWS, pairs, 128), F32),
            pltpu.VMEM((nz, 2, ROWS, pairs, 128), F32),
            pltpu.VMEM((ROWS, pairs, 128), F32),
            pltpu.VMEM((pairs, 8, 128), F32),
            pltpu.VMEM((pairs, 8, 128), F32),
            pltpu.VMEM((2, cross, vel), F32),
            pltpu.VMEM((2, 8, 128), F32),
            pltpu.VMEM((24, vel + 256), BF16),
            dma(()),
            dma((4,)),
            dma(()),
            dma((3,)),
            dma(()),
            dma((3,)),
            dma(()),
            dma((FAN,)),
            dma(()),
            dma(()),
            dma(()),
            dma(()),
            dma(()),
            pltpu.SemaphoreType.REGULAR,
        ],
        compiler_params=pltpu.CompilerParams(
            collective_id=0, has_side_effects=True, vmem_limit_bytes=32 * 1024 * 1024
        ),
    )(
        stay(distribution),
        stay(vel_order.reshape(1, vel)),
        species_mass,
        stay(wall_mask.T),
        stay(inflow_mask.T),
    )
    return pl.pallas_call(
        finish,
        out_shape=jax.ShapeDtypeStruct(distribution.shape, F32),
        in_specs=[vmem] * 4,
        out_specs=hbm,
        scratch_shapes=[pltpu.VMEM((2, cross, vel), F32), dma((3,))],
        compiler_params=pltpu.CompilerParams(vmem_limit_bytes=16 * 1024 * 1024),
    )(*parts)


def solution(mesh):
    in_specs = (
        P("spec", ("groups", "space"), None, "vel"),
        P("vel"),
        P("spec"),
        P(("groups", "space"), None),
        P(("groups", "space"), None),
    )
    out_specs = P("spec", ("groups", "space"), None, "vel")
    return jax.shard_map(
        per_device, mesh=mesh, in_specs=in_specs, out_specs=out_specs, check_vma=False
    )
```

```python
import math

import jax
import jax.numpy as jnp
from jax import lax
from jax.experimental import pallas as pl
from jax.experimental.pallas import tpu as pltpu
from jax.sharding import PartitionSpec as P

NV = 32
NVEL = NV**3
BITS = NV.bit_length() - 1

TIME_STEP = 0.1
RAREFACTION = 0.5
PORT_DENSITY = 1.0
HALF_RANGE = 4.5
CENTRE = (NV - 1) / 2.0
STEP = 2.0 * HALF_RANGE / (NV - 1)
KAPPA = STEP * STEP
LOG2E = math.log2(math.e)

ROOT = 1
ROWS = 6
LOADS = 8
FAN = 4

F32 = jnp.float32
BF16 = jnp.bfloat16
MESH = pl.DeviceIdType.MESH


def pieces(rows):
    high = rows.astype(BF16).astype(F32)
    rest = rows - high
    middle = rest.astype(BF16).astype(F32)
    return jnp.concatenate([high, middle, rest - middle], axis=0).astype(BF16)


def lattice(order):
    index_a = lax.shift_right_logical(order, 2 * BITS).astype(F32)
    index_b = (lax.shift_right_logical(order, BITS) & (NV - 1)).astype(F32)
    index_e = (order & (NV - 1)).astype(F32)
    return index_a - CENTRE, index_b - CENTRE, index_e - CENTRE


def split_square(a, b, e):
    square = a * a + b * b + e * e
    coarse = jnp.floor(square * (1.0 / 32.0)) * 32.0
    return square, coarse, square - coarse


def rows_of(choices, shape):
    row = lax.broadcasted_iota(jnp.int32, shape, 0)
    out = choices[-1]
    for i in range(len(choices) - 2, -1, -1):
        out = jnp.where(row == i, choices[i], out)
    return out


def kernel(
    dist_in, order_in, mass_in, wall_in, inflow_in, coll, inner, lane, flux,
    d, order, mass, wall, inflow, msg, inbox, coef, coef_other, halo_d, halo_c,
    w,
    load_sem, small_sem, msg_send, inbox_sem, coef_send, coef_recv, pass_send,
    halo_d_send, halo_d_recv, halo_c_send, halo_c_recv, halo_r_send, ready,
):
    z, x, s = lax.axis_index("vel"), lax.axis_index("space"), lax.axis_index("spec")
    nz, nx = lax.axis_size("vel"), lax.axis_size("space")
    left, right = lax.rem(x + nx - 1, nx), lax.rem(x + 1, nx)
    slab, cross, vel = d.shape
    pairs = slab // 2
    is_root = (z == 0) & (s == ROOT)
    is_leader = lax.rem(z, FAN) == 0
    leader = z - lax.rem(z, FAN)
    middle = nz // 2 - 1
    following, preceding = z + FAN, z - FAN
    passes = is_leader & (z > 0)
    hands_on = passes & (z < nz - 2 * FAN)
    is_handed = passes & (z != FAN) & (z != nz - FAN)
    is_member = (z > FAN) & (leader != z)
    is_first = z < FAN

    barrier = pltpu.get_barrier_semaphore()

    def signal(sem, **where):
        pl.semaphore_signal(sem, inc=1, device_id=where, device_id_type=MESH)

    def settle(ref, sem):
        pltpu.make_async_copy(ref, ref, sem).wait()

    smalls = [
        pltpu.make_async_copy(order_in, order, small_sem.at[0]),
        pltpu.make_async_copy(mass_in, mass, small_sem.at[1]),
        pltpu.make_async_copy(wall_in, wall, small_sem.at[2]),
        pltpu.make_async_copy(inflow_in, inflow, small_sem.at[3]),
    ]
    loads = [
        pltpu.make_async_copy(
            dist_in.at[0, pl.ds(i, slab // LOADS)], d.at[pl.ds(i, slab // LOADS)], load_sem
        )
        for i in range(0, slab, slab // LOADS)
    ]
    for copy in smalls[:2] + loads + smalls[2:]:
        copy.start()

    signal(barrier, space=left)
    signal(barrier, space=right)

    @pl.when(is_root)
    def _():
        signal(barrier, spec=1 - s)

        def tell(i, carry):
            signal(barrier, vel=i, spec=0)
            signal(barrier, vel=i, spec=1)
            return carry

        lax.fori_loop(1, nz, tell, 0)

    @pl.when(is_first)
    def _():
        signal(barrier, space=left, vel=0, spec=ROOT)
        signal(barrier, space=right, vel=0, spec=ROOT)

    @pl.when(passes)
    def _():
        for k in range(1, FAN):
            signal(barrier, vel=z + k)

    @pl.when(hands_on)
    def _():
        signal(barrier, vel=following)

    smalls[0].wait()
    smalls[1].wait()
    a, b, e = lattice(jnp.broadcast_to(order[...], (8, vel)))
    square, coarse, fine = split_square(a, b, e)
    phi = rows_of([jnp.ones_like(a), jnp.abs(b), a, b, e, coarse, fine, fine], a.shape)
    phi = phi.astype(BF16)

    m = jnp.full((8, 128), mass[0], jnp.int32).astype(F32)
    root_m = jnp.sqrt(m)
    unit = jnp.full((8, 128), 1.0 / NVEL, F32)
    speed = root_m * (STEP / NVEL)
    energy = jnp.full((8, 128), 0.5 * KAPPA / NVEL, F32)
    scale = rows_of([unit, speed, speed, speed, speed, energy, energy, energy], m.shape)
    row = lax.broadcasted_iota(jnp.int32, (8, 128), 0)
    height = lax.broadcasted_iota(jnp.int32, (8, 128), 1) % cross
    amid = (height > 0) & (height < cross - 1)
    nt = (((1,), (1,)), ((), ()))
    settle(d, load_sem)
    for p in range(pairs):
        block = d[2 * p : 2 * p + 2].reshape(2 * cross, vel)
        high = block.astype(BF16)
        low = (block - high.astype(F32)).astype(BF16)
        part = lax.dot_general(phi, high, nt, preferred_element_type=F32)
        part += lax.dot_general(phi, low, nt, preferred_element_type=F32)
        part = (part + jnp.where(row == 5, pltpu.roll(part, 7, 0), 0.0)) * scale
        msg[:, p, :] = jnp.where((row == 1) & amid, m, part)[:ROWS]

    def one(flag):
        return jnp.where(flag, 1, 0)

    pl.semaphore_wait(
        barrier,
        2 + one(jnp.logical_not(is_root)) + one(is_member | is_handed) + 4 * FAN * one(is_root),
    )

    def to_root():
        return pltpu.make_async_remote_copy(
            src_ref=msg,
            dst_ref=inbox.at[z, s],
            send_sem=msg_send,
            recv_sem=inbox_sem.at[one(z > 0) + one(z > middle)],
            device_id={"vel": 0, "spec": ROOT},
            device_id_type=MESH,
        )

    @pl.when(jnp.logical_not(is_root))
    def _():
        to_root().start()

    def halo_copy(src, box, sends, recvs, side):
        return pltpu.make_async_remote_copy(
            src_ref=src,
            dst_ref=box.at[side],
            send_sem=sends,
            recv_sem=recvs,
            device_id={"space": right if side == 0 else left},
            device_id_type=MESH,
        )

    halo_ds = [
        halo_copy(d.at[slab - 1], halo_d, halo_d_send, halo_d_recv, 0),
        halo_copy(d.at[0], halo_d, halo_d_send, halo_d_recv, 1),
    ]
    for copy in halo_ds:
        copy.start()

    @pl.when(is_member | is_handed)
    def _():
        signal(ready, vel=jnp.where(is_handed, preceding, leader))

    speed_unit = (STEP / root_m)[:, :1]
    ones = jnp.ones((8, vel), F32)
    zeros = jnp.zeros((8, 128), F32)
    table = rows_of([ones, a, b, e, coarse, fine, 0.0 * ones, 0.0 * ones], ones.shape)
    keep = jnp.where(row == 6, 1.0, zeros)
    emit = jnp.where(row == 7, 1.0, zeros)
    table = jnp.concatenate([table, keep, emit], axis=1)
    w[...] = jnp.concatenate([table, table, table], axis=0).astype(BF16)
    go_x = TIME_STEP * speed_unit * jnp.abs(a)
    go_y = TIME_STEP * speed_unit * jnp.abs(b)
    law_unit = NVEL * (KAPPA / (2.0 * math.pi)) ** 1.5
    law = law_unit * jnp.exp(-0.5 * KAPPA * square)
    lane[...] = rows_of([1.0 - go_x - go_y, go_x, go_y, a, b, law, law, law], ones.shape)

    def coef_copy(i, core, own, sem):
        return pltpu.make_async_remote_copy(
            src_ref=coef if own else coef_other,
            dst_ref=coef,
            send_sem=sem,
            recv_sem=coef_recv,
            device_id={"vel": i, "spec": core},
            device_id_type=MESH,
        )

    def served(places, sem):
        nearest = sorted(places, key=lambda i: min(i, nz - i))
        return [coef_copy(i, core, core == ROOT, sem) for i in nearest for core in (ROOT, 1 - ROOT)]

    first, others, leaders = range(1, 2), range(2, FAN), sorted({FAN, nz - FAN})

    def borders(places):
        return [
            pltpu.make_async_remote_copy(
                src_ref=(coef if core == ROOT else coef_other).at[pairs - 1 if side == 0 else 0],
                dst_ref=halo_c.at[side],
                send_sem=halo_r_send,
                recv_sem=halo_c_recv,
                device_id={"space": right if side == 0 else left, "vel": i, "spec": core},
                device_id_type=MESH,
            )
            for i in places
            for core in (ROOT, 1 - ROOT)
            for side in range(2)
        ]


    @pl.when(is_root)
    def _():
        for copy in smalls[2:]:
            copy.wait()
        shape = (pairs, 128)
        spot = lax.broadcasted_iota(jnp.int32, shape, 0) * 128
        spot = spot + lax.broadcasted_iota(jnp.int32, shape, 1)
        wall_row = jnp.zeros(shape, F32)
        port_row = jnp.zeros(shape, F32)
        for i in range(slab):
            for side in range(2):
                here = spot == i * cross + side * (cross - 1)
                wall_row = jnp.where(here, jnp.full(shape, wall[side, i], jnp.int32).astype(F32), wall_row)
                port_row = jnp.where(here, jnp.full(shape, inflow[side, i], jnp.int32).astype(F32), port_row)
        port_row = port_row * PORT_DENSITY
        offset = spot.astype(F32) - CENTRE
        bell = jnp.where(spot < NV, jnp.exp(-0.5 * KAPPA * offset * offset), 0.0)
        bell_sum = jnp.sum(jnp.sum(bell, axis=1, keepdims=True), axis=0, keepdims=True)
        flow = jnp.maximum(offset, 0.0) * bell
        flow_sum = jnp.sum(jnp.sum(flow, axis=1, keepdims=True), axis=0, keepdims=True)
        sign = jnp.where(lax.rem(spot, cross) == 0, -1.0, 1.0)
        law_scale = (2.0 * STEP) * (KAPPA / (2.0 * math.pi)) ** 1.5 * flow_sum * bell_sum * bell_sum

        settle(inbox.at[0, 1 - ROOT], inbox_sem.at[0])
        mine, partner = msg[...], inbox[0, 1 - ROOT]
        spot_b = lax.rem(spot, cross)
        between = (spot_b > 0) & (spot_b < cross - 1)
        masses = []
        for part in (mine, partner):
            found = jnp.where(between, part[1], 0.0)
            found = jnp.max(jnp.max(found, axis=1, keepdims=True), axis=0, keepdims=True)
            masses.append(jnp.broadcast_to(found, shape))
        spacings = [STEP / jnp.sqrt(v) for v in masses]
        walls = [wall_row / (jnp.sqrt(v) * law_scale) for v in masses]
        volumes = [
            (TIME_STEP / RAREFACTION) * NVEL * v * v * v * (0.5 / math.pi) for v in spacings
        ]

        own, other = mine, partner
        for part, (low, high) in enumerate([(1, middle + 1), (middle + 1, nz)]):
            settle(inbox.at[pl.ds(low, high - low)], inbox_sem.at[part + 1])
            for i in range(low, high):
                own += inbox[i, ROOT]
                other += inbox[i, 1 - ROOT]

        density = own[0] + other[0]
        per_density = 1.0 / density
        weight = masses[0] * own[0] + masses[1] * other[0]
        per_weight = 1.0 / weight
        flow_x = (own[2] + other[2]) * per_weight
        flow_y = (own[3] + other[3]) * per_weight
        flow_z = (own[4] + other[4]) * per_weight
        flow_square = flow_x * flow_x + flow_y * flow_y + flow_z * flow_z
        heat = 2.0 / 3.0 * (own[5] + other[5] - 0.5 * weight * flow_square) * per_density
        per_heat = 1.0 / heat
        for part, v, h, wall_v, volume, box in (
            (own, masses[0], spacings[0], walls[0], volumes[0], coef),
            (other, masses[1], spacings[1], walls[1], volumes[1], coef_other),
        ):
            sharp = v * per_heat
            top = part[0] * density * volume * sharp * jnp.sqrt(sharp * (0.5 / math.pi))
            slope = LOG2E * h * sharp
            curve = -0.5 * h * slope
            rows = [
                LOG2E * (jnp.log(top) - 0.5 * sharp * flow_square),
                slope * flow_x,
                slope * flow_y,
                slope * flow_z,
                curve,
                curve,
                1.0 - (TIME_STEP / RAREFACTION) * density,
                wall_v * (part[1] + sign * part[3]) + port_row,
            ]
            for i, values in enumerate(rows):
                box[:, i, :] = values

        coef_copy(0, 1 - ROOT, False, coef_send.at[0]).start()
        for copy in borders(range(1)) + served(first, coef_send.at[1]) + borders(first):
            copy.start()

    @pl.when(jnp.logical_not(is_root))
    def _():
        settle(coef, coef_recv)

    halo_cs = [
        halo_copy(coef.at[pairs - 1], halo_c, halo_c_send, halo_c_recv, 0),
        halo_copy(coef.at[0], halo_c, halo_c_send, halo_c_recv, 1),
    ]

    @pl.when(jnp.logical_not(is_first))
    def _():
        for copy in halo_cs:
            copy.start()

    def pass_on():
        return [coef_copy(z + k, s, True, pass_send.at[k - 1]) for k in range(1, FAN)]

    def hand_on():
        return coef_copy(following, s, True, pass_send.at[FAN - 1])

    @pl.when(passes)
    def _():
        pl.semaphore_wait(ready, FAN - 1 + one(hands_on))
        for copy in pass_on():
            copy.start()

    @pl.when(hands_on)
    def _():
        hand_on().start()

    tn = (((0,), (0,)), ((), ()))
    width = 256

    def collide(parts, rows, put, put_flux):
        side = lax.dot_general(parts, w[:, vel : vel + 256], tn, preferred_element_type=F32)
        stay = jnp.concatenate([side[:, :128]] * (width // 128), axis=1)
        if put_flux is not None:
            put_flux(side[:, 128:].reshape(2, cross, 128))
        for c in range(0, vel, width):
            power = lax.dot_general(parts, w[:, c : c + width], tn, preferred_element_type=F32)
            old = rows(c).reshape(2 * cross, width)
            put(c, (old * stay + jnp.exp2(power)).reshape(2, cross, width))

    for p in range(pairs):

        def rows(c, p=p):
            return d[2 * p : 2 * p + 2, :, c : c + width]

        def put(c, value, p=p):
            coll[2 * p + 1 : 2 * p + 3, :, c : c + width] = value

        def put_flux(value, p=p):
            flux[2 * p : 2 * p + 2] = value

        collide(pieces(coef[p]), rows, put, put_flux)

    @pl.when(is_root)
    def _():
        beyond = served(leaders, coef_send.at[2])
        for copy in served(others, coef_send.at[1]) + borders(others) + beyond:
            copy.start()

    for i in range(1, slab - 1):
        stream(coll, lane, flux, i, inner.at[i - 1])

    settle(halo_d, halo_d_recv)
    settle(halo_c, halo_c_recv)
    spot = lax.broadcasted_iota(jnp.int32, (8, 128), 1)
    outer = jnp.where(spot < cross, halo_c[1], halo_c[0])

    def rows(c):
        return jnp.concatenate([halo_d[1:2, :, c : c + width], halo_d[0:1, :, c : c + width]], 0)

    def put(c, value):
        coll[slab + 1, :, c : c + width] = value[0]
        coll[0, :, c : c + width] = value[1]

    collide(pieces(outer), rows, put, None)

    settle(halo_d, halo_d_send)

    @pl.when(jnp.logical_not(is_first))
    def _():
        settle(halo_c, halo_c_send)

    @pl.when(jnp.logical_not(is_root))
    def _():
        settle(msg, msg_send)
        for copy in smalls[2:]:
            copy.wait()

    @pl.when(is_root)
    def _():
        settle(coef, coef_send.at[0])
        settle(d.at[0, pl.ds(0, 8 * (FAN - 1))], coef_send.at[1])
        settle(d.at[0, pl.ds(0, 8 * len(leaders))], coef_send.at[2])
        settle(d.at[0, pl.ds(0, 4 * FAN)], halo_r_send)

    @pl.when(passes)
    def _():
        for copy in pass_on():
            copy.wait_send()

    @pl.when(hands_on)
    def _():
        hand_on().wait_send()


def stream(coll, lane, flux, i, out):
    _, cross, vel = coll.shape
    level = lax.broadcasted_iota(jnp.int32, (cross, 128), 0)
    low_flux = flux[i, 0:1]
    high_flux = flux[i, cross - 1 : cross]
    for c in range(0, vel, 128):
        cols = slice(c, c + 128)
        here = coll[i + 1, :, cols]
        law = lane[5:6, cols]
        below = jnp.where(level == 0, low_flux * law, pltpu.roll(here, 1, 0))
        above = jnp.where(level == cross - 1, high_flux * law, pltpu.roll(here, cross - 1, 0))
        beside = jnp.where(lane[3:4, cols] > 0.0, coll[i, :, cols], coll[i + 2, :, cols])
        over = jnp.where(lane[4:5, cols] > 0.0, below, above)
        out[:, cols] = lane[0:1, cols] * here + lane[1:2, cols] * beside + lane[2:3, cols] * over


def finish(coll, inner, lane, flux, out, edge, sem):
    slab = flux.shape[0]
    for i in range(slab - 2):
        pltpu.make_async_copy(inner.at[i], out.at[0, i + 1], sem.at[2]).start()
    copies = [pltpu.make_async_copy(inner, out.at[0, pl.ds(1, slab - 2)], sem.at[2])]
    for k, i in enumerate((0, slab - 1)):
        stream(coll, lane, flux, i, edge.at[k])
        copies.append(pltpu.make_async_copy(edge.at[k], out.at[0, i], sem.at[k]))
        copies[-1].start()
    for copy in copies:
        copy.wait()


def per_device(distribution, vel_order, species_mass, wall_mask, inflow_mask):
    _, slab, cross, vel = distribution.shape
    nz = lax.axis_size("vel")
    pairs = slab // 2
    hbm = pl.BlockSpec(memory_space=pltpu.HBM)

    def stay(array):
        return pltpu.with_memory_space_constraint(array, pltpu.HBM)

    dma = pltpu.SemaphoreType.DMA
    vmem = pl.BlockSpec(memory_space=pltpu.VMEM)
    passed = [
        jax.ShapeDtypeStruct(shape, F32)
        for shape in [
            (slab + 2, cross, vel),
            (slab - 2, cross, vel),
            (8, vel),
            (slab, cross, 128),
        ]
    ]
    parts = pl.pallas_call(
        kernel,
        out_shape=passed,
        in_specs=[hbm] * 5,
        out_specs=[vmem] * 4,
        scratch_shapes=[
            pltpu.VMEM((slab, cross, vel), F32),
            pltpu.VMEM((1, vel), jnp.int32),
            pltpu.SMEM(species_mass.shape, jnp.int32),
            pltpu.SMEM((2, slab), jnp.int32),
            pltpu.SMEM((2, slab), jnp.int32),
            pltpu.VMEM((ROWS, pairs, 128), F32),
            pltpu.VMEM((nz, 2, ROWS, pairs, 128), F32),
            pltpu.VMEM((pairs, 8, 128), F32),
            pltpu.VMEM((pairs, 8, 128), F32),
            pltpu.VMEM((2, cross, vel), F32),
            pltpu.VMEM((2, 8, 128), F32),
            pltpu.VMEM((24, vel + 256), BF16),
            dma(()),
            dma((4,)),
            dma(()),
            dma((3,)),
            dma((3,)),
            dma(()),
            dma((FAN,)),
            dma(()),
            dma(()),
            dma(()),
            dma(()),
            dma(()),
            pltpu.SemaphoreType.REGULAR,
        ],
        compiler_params=pltpu.CompilerParams(
            collective_id=0, has_side_effects=True, vmem_limit_bytes=32 * 1024 * 1024
        ),
    )(
        stay(distribution),
        stay(vel_order.reshape(1, vel)),
        species_mass,
        stay(wall_mask.T),
        stay(inflow_mask.T),
    )
    return pl.pallas_call(
        finish,
        out_shape=jax.ShapeDtypeStruct(distribution.shape, F32),
        in_specs=[vmem] * 4,
        out_specs=hbm,
        scratch_shapes=[pltpu.VMEM((2, cross, vel), F32), dma((3,))],
        compiler_params=pltpu.CompilerParams(vmem_limit_bytes=16 * 1024 * 1024),
    )(*parts)


def solution(mesh):
    in_specs = (
        P("spec", ("groups", "space"), None, "vel"),
        P("vel"),
        P("spec"),
        P(("groups", "space"), None),
        P(("groups", "space"), None),
    )
    out_specs = P("spec", ("groups", "space"), None, "vel")
    return jax.shard_map(
        per_device, mesh=mesh, in_specs=in_specs, out_specs=out_specs, check_vma=False
    )
```

```python
import math

import jax
import jax.numpy as jnp
from jax import lax
from jax.experimental import pallas as pl
from jax.experimental.pallas import tpu as pltpu
from jax.sharding import PartitionSpec as P

NV = 32
NVEL = NV**3
BITS = NV.bit_length() - 1

TIME_STEP = 0.1
RAREFACTION = 0.5
PORT_DENSITY = 1.0
HALF_RANGE = 4.5
CENTRE = (NV - 1) / 2.0
STEP = 2.0 * HALF_RANGE / (NV - 1)
KAPPA = STEP * STEP
LOG2E = math.log2(math.e)

ROOT = 1
ROWS = 6
LOADS = 8
FAN = 4

F32 = jnp.float32
BF16 = jnp.bfloat16
MESH = pl.DeviceIdType.MESH


def pieces(rows):
    high = rows.astype(BF16).astype(F32)
    rest = rows - high
    middle = rest.astype(BF16).astype(F32)
    return jnp.concatenate([high, middle, rest - middle], axis=0).astype(BF16)


def lattice(order):
    index_a = lax.shift_right_logical(order, 2 * BITS).astype(F32)
    index_b = (lax.shift_right_logical(order, BITS) & (NV - 1)).astype(F32)
    index_e = (order & (NV - 1)).astype(F32)
    return index_a - CENTRE, index_b - CENTRE, index_e - CENTRE


def split_square(a, b, e):
    square = a * a + b * b + e * e
    coarse = jnp.floor(square * (1.0 / 32.0)) * 32.0
    return square, coarse, square - coarse


def rows_of(choices, shape):
    row = lax.broadcasted_iota(jnp.int32, shape, 0)
    out = choices[-1]
    for i in range(len(choices) - 2, -1, -1):
        out = jnp.where(row == i, choices[i], out)
    return out


def kernel(
    dist_in, order_in, mass_in, wall_in, inflow_in, coll, inner, lane, flux,
    d, order, mass, wall, inflow, msg, inbox, coef, coef_other, halo_d, halo_c,
    w,
    load_sem, small_sem, msg_send, inbox_sem, coef_send, coef_recv, pass_send,
    halo_d_send, halo_d_recv, halo_c_send, halo_c_recv, halo_r_send, ready,
):
    z, x, s = lax.axis_index("vel"), lax.axis_index("space"), lax.axis_index("spec")
    nz, nx = lax.axis_size("vel"), lax.axis_size("space")
    left, right = lax.rem(x + nx - 1, nx), lax.rem(x + 1, nx)
    slab, cross, vel = d.shape
    pairs = slab // 2
    is_root = (z == 0) & (s == ROOT)
    is_leader = lax.rem(z, FAN) == 0
    leader = z - lax.rem(z, FAN)
    middle = nz // 2 - 1
    following, preceding = z + FAN, z - FAN
    passes = is_leader & (z > 0)
    hands_on = passes & (z < nz - 2 * FAN)
    is_handed = passes & (z != FAN) & (z != nz - FAN)
    is_member = (z > FAN) & (leader != z)
    is_first = z < FAN

    barrier = pltpu.get_barrier_semaphore()

    def signal(sem, **where):
        pl.semaphore_signal(sem, inc=1, device_id=where, device_id_type=MESH)

    def settle(ref, sem):
        pltpu.make_async_copy(ref, ref, sem).wait()

    smalls = [
        pltpu.make_async_copy(order_in, order, small_sem.at[0]),
        pltpu.make_async_copy(mass_in, mass, small_sem.at[1]),
        pltpu.make_async_copy(wall_in, wall, small_sem.at[2]),
        pltpu.make_async_copy(inflow_in, inflow, small_sem.at[3]),
    ]
    loads = [
        pltpu.make_async_copy(
            dist_in.at[0, pl.ds(i, slab // LOADS)], d.at[pl.ds(i, slab // LOADS)], load_sem
        )
        for i in range(0, slab, slab // LOADS)
    ]
    for copy in smalls[:2] + loads + smalls[2:]:
        copy.start()

    signal(barrier, space=left)
    signal(barrier, space=right)

    @pl.when(is_root)
    def _():
        signal(barrier, spec=1 - s)

        def tell(i, carry):
            signal(barrier, vel=i, spec=0)
            signal(barrier, vel=i, spec=1)
            return carry

        lax.fori_loop(1, nz, tell, 0)

    @pl.when(is_first)
    def _():
        signal(barrier, space=left, vel=0, spec=ROOT)
        signal(barrier, space=right, vel=0, spec=ROOT)

    @pl.when(passes)
    def _():
        for k in range(1, FAN):
            signal(barrier, vel=z + k)

    @pl.when(hands_on)
    def _():
        signal(barrier, vel=following)

    smalls[0].wait()
    smalls[1].wait()
    a, b, e = lattice(jnp.broadcast_to(order[...], (8, vel)))
    square, coarse, fine = split_square(a, b, e)
    phi = rows_of([jnp.ones_like(a), jnp.abs(b), a, b, e, coarse, fine, fine], a.shape)
    phi = phi.astype(BF16)

    m = jnp.full((8, 128), mass[0], jnp.int32).astype(F32)
    root_m = jnp.sqrt(m)
    unit = jnp.full((8, 128), 1.0 / NVEL, F32)
    speed = root_m * (STEP / NVEL)
    energy = jnp.full((8, 128), 0.5 * KAPPA / NVEL, F32)
    scale = rows_of([unit, speed, speed, speed, speed, energy, energy, energy], m.shape)
    row = lax.broadcasted_iota(jnp.int32, (8, 128), 0)
    height = lax.broadcasted_iota(jnp.int32, (8, 128), 1) % cross
    amid = (height > 0) & (height < cross - 1)
    nt = (((1,), (1,)), ((), ()))
    settle(d, load_sem)
    for p in range(pairs):
        block = d[2 * p : 2 * p + 2].reshape(2 * cross, vel)
        high = block.astype(BF16)
        low = (block - high.astype(F32)).astype(BF16)
        part = lax.dot_general(phi, high, nt, preferred_element_type=F32)
        part += lax.dot_general(phi, low, nt, preferred_element_type=F32)
        part = (part + jnp.where(row == 5, pltpu.roll(part, 7, 0), 0.0)) * scale
        msg[:, p, :] = jnp.where((row == 1) & amid, m, part)[:ROWS]

    def one(flag):
        return jnp.where(flag, 1, 0)

    pl.semaphore_wait(
        barrier,
        2 + one(jnp.logical_not(is_root)) + one(is_member | is_handed) + 4 * FAN * one(is_root),
    )

    def to_root():
        return pltpu.make_async_remote_copy(
            src_ref=msg,
            dst_ref=inbox.at[z, s],
            send_sem=msg_send,
            recv_sem=inbox_sem.at[one(z > 0) + one(z > middle) + one(z >= nz - FAN)],
            device_id={"vel": 0, "spec": ROOT},
            device_id_type=MESH,
        )

    @pl.when(jnp.logical_not(is_root))
    def _():
        to_root().start()

    def halo_copy(src, box, sends, recvs, side):
        return pltpu.make_async_remote_copy(
            src_ref=src,
            dst_ref=box.at[side],
            send_sem=sends,
            recv_sem=recvs,
            device_id={"space": right if side == 0 else left},
            device_id_type=MESH,
        )

    halo_ds = [
        halo_copy(d.at[slab - 1], halo_d, halo_d_send, halo_d_recv, 0),
        halo_copy(d.at[0], halo_d, halo_d_send, halo_d_recv, 1),
    ]
    for copy in halo_ds:
        copy.start()

    @pl.when(is_member | is_handed)
    def _():
        signal(ready, vel=jnp.where(is_handed, preceding, leader))

    speed_unit = (STEP / root_m)[:, :1]
    ones = jnp.ones((8, vel), F32)
    zeros = jnp.zeros((8, 128), F32)
    table = rows_of([ones, a, b, e, coarse, fine, 0.0 * ones, 0.0 * ones], ones.shape)
    keep = jnp.where(row == 6, 1.0, zeros)
    emit = jnp.where(row == 7, 1.0, zeros)
    table = jnp.concatenate([table, keep, emit], axis=1)
    w[...] = jnp.concatenate([table, table, table], axis=0).astype(BF16)
    go_x = TIME_STEP * speed_unit * jnp.abs(a)
    go_y = TIME_STEP * speed_unit * jnp.abs(b)
    law_unit = NVEL * (KAPPA / (2.0 * math.pi)) ** 1.5
    law = law_unit * jnp.exp(-0.5 * KAPPA * square)
    lane[...] = rows_of([1.0 - go_x - go_y, go_x, go_y, a, b, law, law, law], ones.shape)

    def coef_copy(i, core, own, sem):
        return pltpu.make_async_remote_copy(
            src_ref=coef if own else coef_other,
            dst_ref=coef,
            send_sem=sem,
            recv_sem=coef_recv,
            device_id={"vel": i, "spec": core},
            device_id_type=MESH,
        )

    def served(places, sem):
        nearest = sorted(places, key=lambda i: min(i, nz - i))
        return [coef_copy(i, core, core == ROOT, sem) for i in nearest for core in (ROOT, 1 - ROOT)]

    first, others, leaders = range(1, 2), range(2, FAN), sorted({FAN, nz - FAN})

    def borders(places, cores=(ROOT, 1 - ROOT)):
        return [
            pltpu.make_async_remote_copy(
                src_ref=(coef if core == ROOT else coef_other).at[pairs - 1 if side == 0 else 0],
                dst_ref=halo_c.at[side],
                send_sem=halo_r_send,
                recv_sem=halo_c_recv,
                device_id={"space": right if side == 0 else left, "vel": i, "spec": core},
                device_id_type=MESH,
            )
            for i in places
            for core in cores
            for side in range(2)
        ]


    @pl.when(is_root)
    def _():
        for copy in smalls[2:]:
            copy.wait()
        shape = (pairs, 128)
        spot = lax.broadcasted_iota(jnp.int32, shape, 0) * 128
        spot = spot + lax.broadcasted_iota(jnp.int32, shape, 1)
        wall_row = jnp.zeros(shape, F32)
        port_row = jnp.zeros(shape, F32)
        for i in range(slab):
            for side in range(2):
                here = spot == i * cross + side * (cross - 1)
                wall_row = jnp.where(here, jnp.full(shape, wall[side, i], jnp.int32).astype(F32), wall_row)
                port_row = jnp.where(here, jnp.full(shape, inflow[side, i], jnp.int32).astype(F32), port_row)
        port_row = port_row * PORT_DENSITY
        offset = spot.astype(F32) - CENTRE
        bell = jnp.where(spot < NV, jnp.exp(-0.5 * KAPPA * offset * offset), 0.0)
        bell_sum = jnp.sum(jnp.sum(bell, axis=1, keepdims=True), axis=0, keepdims=True)
        flow = jnp.maximum(offset, 0.0) * bell
        flow_sum = jnp.sum(jnp.sum(flow, axis=1, keepdims=True), axis=0, keepdims=True)
        sign = jnp.where(lax.rem(spot, cross) == 0, -1.0, 1.0)
        law_scale = (2.0 * STEP) * (KAPPA / (2.0 * math.pi)) ** 1.5 * flow_sum * bell_sum * bell_sum

        settle(inbox.at[0, 1 - ROOT], inbox_sem.at[0])
        mine, partner = msg[...], inbox[0, 1 - ROOT]
        spot_b = lax.rem(spot, cross)
        between = (spot_b > 0) & (spot_b < cross - 1)
        masses = []
        for part in (mine, partner):
            found = jnp.where(between, part[1], 0.0)
            found = jnp.max(jnp.max(found, axis=1, keepdims=True), axis=0, keepdims=True)
            masses.append(jnp.broadcast_to(found, shape))
        spacings = [STEP / jnp.sqrt(v) for v in masses]
        walls = [wall_row / (jnp.sqrt(v) * law_scale) for v in masses]
        volumes = [
            (TIME_STEP / RAREFACTION) * NVEL * v * v * v * (0.5 / math.pi) for v in spacings
        ]

        own, other = mine, partner
        for part, (low, high) in enumerate([(1, middle + 1), (middle + 1, nz - FAN), (nz - FAN, nz)]):
            settle(inbox.at[pl.ds(low, high - low)], inbox_sem.at[part + 1])
            for i in range(low, high):
                own += inbox[i, ROOT]
                other += inbox[i, 1 - ROOT]

        density = own[0] + other[0]
        per_density = 1.0 / density
        weight = masses[0] * own[0] + masses[1] * other[0]
        per_weight = 1.0 / weight
        flow_x = (own[2] + other[2]) * per_weight
        flow_y = (own[3] + other[3]) * per_weight
        flow_z = (own[4] + other[4]) * per_weight
        flow_square = flow_x * flow_x + flow_y * flow_y + flow_z * flow_z
        heat = 2.0 / 3.0 * (own[5] + other[5] - 0.5 * weight * flow_square) * per_density
        per_heat = 1.0 / heat
        for part, v, h, wall_v, volume, box in (
            (own, masses[0], spacings[0], walls[0], volumes[0], coef),
            (other, masses[1], spacings[1], walls[1], volumes[1], coef_other),
        ):
            sharp = v * per_heat
            top = part[0] * density * volume * sharp * jnp.sqrt(sharp * (0.5 / math.pi))
            slope = LOG2E * h * sharp
            curve = -0.5 * h * slope
            rows = [
                LOG2E * (jnp.log(top) - 0.5 * sharp * flow_square),
                slope * flow_x,
                slope * flow_y,
                slope * flow_z,
                curve,
                curve,
                1.0 - (TIME_STEP / RAREFACTION) * density,
                wall_v * (part[1] + sign * part[3]) + port_row,
            ]
            for i, values in enumerate(rows):
                box[:, i, :] = values
            if box is coef:
                for copy in borders(range(1), (ROOT,)):
                    copy.start()

        coef_copy(0, 1 - ROOT, False, coef_send.at[0]).start()
        for copy in (
            borders(range(1), (1 - ROOT,)) + served(first, coef_send.at[1]) + borders(first)
        ):
            copy.start()

    @pl.when(jnp.logical_not(is_root))
    def _():
        settle(coef, coef_recv)

    halo_cs = [
        halo_copy(coef.at[pairs - 1], halo_c, halo_c_send, halo_c_recv, 0),
        halo_copy(coef.at[0], halo_c, halo_c_send, halo_c_recv, 1),
    ]

    @pl.when(jnp.logical_not(is_first))
    def _():
        for copy in halo_cs:
            copy.start()

    def pass_on():
        return [coef_copy(z + k, s, True, pass_send.at[k - 1]) for k in range(1, FAN)]

    def hand_on():
        return coef_copy(following, s, True, pass_send.at[FAN - 1])

    @pl.when(passes)
    def _():
        pl.semaphore_wait(ready, FAN - 1 + one(hands_on))
        for copy in pass_on():
            copy.start()

    @pl.when(hands_on)
    def _():
        hand_on().start()

    tn = (((0,), (0,)), ((), ()))
    width = 256

    def collide(parts, rows, put, put_flux):
        side = lax.dot_general(parts, w[:, vel : vel + 256], tn, preferred_element_type=F32)
        stay = jnp.concatenate([side[:, :128]] * (width // 128), axis=1)
        if put_flux is not None:
            put_flux(side[:, 128:].reshape(2, cross, 128))
        for c in range(0, vel, width):
            power = lax.dot_general(parts, w[:, c : c + width], tn, preferred_element_type=F32)
            old = rows(c).reshape(2 * cross, width)
            put(c, (old * stay + jnp.exp2(power)).reshape(2, cross, width))

    for p in range(pairs):

        def rows(c, p=p):
            return d[2 * p : 2 * p + 2, :, c : c + width]

        def put(c, value, p=p):
            coll[2 * p + 1 : 2 * p + 3, :, c : c + width] = value

        def put_flux(value, p=p):
            flux[2 * p : 2 * p + 2] = value

        collide(pieces(coef[p]), rows, put, put_flux)

    @pl.when(is_root)
    def _():
        beyond = served(leaders, coef_send.at[2])
        for copy in served(others, coef_send.at[1]) + borders(others) + beyond:
            copy.start()

    for i in range(1, slab - 1):
        stream(coll, lane, flux, i, inner.at[i - 1])

    settle(halo_d, halo_d_recv)
    settle(halo_c, halo_c_recv)
    spot = lax.broadcasted_iota(jnp.int32, (8, 128), 1)
    outer = jnp.where(spot < cross, halo_c[1], halo_c[0])

    def rows(c):
        return jnp.concatenate([halo_d[1:2, :, c : c + width], halo_d[0:1, :, c : c + width]], 0)

    def put(c, value):
        coll[slab + 1, :, c : c + width] = value[0]
        coll[0, :, c : c + width] = value[1]

    collide(pieces(outer), rows, put, None)

    settle(halo_d, halo_d_send)

    @pl.when(jnp.logical_not(is_first))
    def _():
        settle(halo_c, halo_c_send)

    @pl.when(jnp.logical_not(is_root))
    def _():
        settle(msg, msg_send)
        for copy in smalls[2:]:
            copy.wait()

    @pl.when(is_root)
    def _():
        settle(coef, coef_send.at[0])
        settle(d.at[0, pl.ds(0, 8 * (FAN - 1))], coef_send.at[1])
        settle(d.at[0, pl.ds(0, 8 * len(leaders))], coef_send.at[2])
        settle(d.at[0, pl.ds(0, 4 * FAN)], halo_r_send)

    @pl.when(passes)
    def _():
        for copy in pass_on():
            copy.wait_send()

    @pl.when(hands_on)
    def _():
        hand_on().wait_send()


def stream(coll, lane, flux, i, out):
    _, cross, vel = coll.shape
    level = lax.broadcasted_iota(jnp.int32, (cross, 128), 0)
    low_flux = flux[i, 0:1]
    high_flux = flux[i, cross - 1 : cross]
    for c in range(0, vel, 128):
        cols = slice(c, c + 128)
        here = coll[i + 1, :, cols]
        law = lane[5:6, cols]
        below = jnp.where(level == 0, low_flux * law, pltpu.roll(here, 1, 0))
        above = jnp.where(level == cross - 1, high_flux * law, pltpu.roll(here, cross - 1, 0))
        beside = jnp.where(lane[3:4, cols] > 0.0, coll[i, :, cols], coll[i + 2, :, cols])
        over = jnp.where(lane[4:5, cols] > 0.0, below, above)
        out[:, cols] = lane[0:1, cols] * here + lane[1:2, cols] * beside + lane[2:3, cols] * over


def finish(coll, inner, lane, flux, out, edge, sem):
    slab = flux.shape[0]
    for i in range(slab - 2):
        pltpu.make_async_copy(inner.at[i], out.at[0, i + 1], sem.at[2]).start()
    copies = [pltpu.make_async_copy(inner, out.at[0, pl.ds(1, slab - 2)], sem.at[2])]
    for k, i in enumerate((0, slab - 1)):
        stream(coll, lane, flux, i, edge.at[k])
        copies.append(pltpu.make_async_copy(edge.at[k], out.at[0, i], sem.at[k]))
        copies[-1].start()
    for copy in copies:
        copy.wait()


def per_device(distribution, vel_order, species_mass, wall_mask, inflow_mask):
    _, slab, cross, vel = distribution.shape
    nz = lax.axis_size("vel")
    pairs = slab // 2
    hbm = pl.BlockSpec(memory_space=pltpu.HBM)

    def stay(array):
        return pltpu.with_memory_space_constraint(array, pltpu.HBM)

    dma = pltpu.SemaphoreType.DMA
    vmem = pl.BlockSpec(memory_space=pltpu.VMEM)
    passed = [
        jax.ShapeDtypeStruct(shape, F32)
        for shape in [
            (slab + 2, cross, vel),
            (slab - 2, cross, vel),
            (8, vel),
            (slab, cross, 128),
        ]
    ]
    parts = pl.pallas_call(
        kernel,
        out_shape=passed,
        in_specs=[hbm] * 5,
        out_specs=[vmem] * 4,
        scratch_shapes=[
            pltpu.VMEM((slab, cross, vel), F32),
            pltpu.VMEM((1, vel), jnp.int32),
            pltpu.SMEM(species_mass.shape, jnp.int32),
            pltpu.SMEM((2, slab), jnp.int32),
            pltpu.SMEM((2, slab), jnp.int32),
            pltpu.VMEM((ROWS, pairs, 128), F32),
            pltpu.VMEM((nz, 2, ROWS, pairs, 128), F32),
            pltpu.VMEM((pairs, 8, 128), F32),
            pltpu.VMEM((pairs, 8, 128), F32),
            pltpu.VMEM((2, cross, vel), F32),
            pltpu.VMEM((2, 8, 128), F32),
            pltpu.VMEM((24, vel + 256), BF16),
            dma(()),
            dma((4,)),
            dma(()),
            dma((4,)),
            dma((3,)),
            dma(()),
            dma((FAN,)),
            dma(()),
            dma(()),
            dma(()),
            dma(()),
            dma(()),
            pltpu.SemaphoreType.REGULAR,
        ],
        compiler_params=pltpu.CompilerParams(
            collective_id=0, has_side_effects=True, vmem_limit_bytes=32 * 1024 * 1024
        ),
    )(
        stay(distribution),
        stay(vel_order.reshape(1, vel)),
        species_mass,
        stay(wall_mask.T),
        stay(inflow_mask.T),
    )
    return pl.pallas_call(
        finish,
        out_shape=jax.ShapeDtypeStruct(distribution.shape, F32),
        in_specs=[vmem] * 4,
        out_specs=hbm,
        scratch_shapes=[pltpu.VMEM((2, cross, vel), F32), dma((3,))],
        compiler_params=pltpu.CompilerParams(vmem_limit_bytes=16 * 1024 * 1024),
    )(*parts)


def solution(mesh):
    in_specs = (
        P("spec", ("groups", "space"), None, "vel"),
        P("vel"),
        P("spec"),
        P(("groups", "space"), None),
        P(("groups", "space"), None),
    )
    out_specs = P("spec", ("groups", "space"), None, "vel")
    return jax.shard_map(
        per_device, mesh=mesh, in_specs=in_specs, out_specs=out_specs, check_vma=False
    )
```
